8 devices in a mesh: tp: 2 (over z, y), dp: 4 (over x, core).
Axes of the slice: x: 2, y: 2, z: 1, core: 2. Of those that a mesh axis runs over, the one named last changes fastest.
Arguments:
- hidden: bfloat16 [4, 512, 1024], P('dp')
- residual: float32 [4, 512, 1024], P('dp')
- targets: int32 [4, 512], P('dp')
- embedding: bfloat16 [50280, 1024], P('tp')
- norm_w: float32 [1024], replicated
Outputs:
- output 1: float32 [], replicated
- output 2: float32 [4, 512, 1024], P('dp')
- output 3: float32 [50280, 1024], P('tp')
- output 4: float32 [1024], replicated
All inputs are finite; a program needn't handle non-finite values.
Results may differ from the reference program's by a relative error of at most 0.001.
Values sent between devices are 32-bit elements.
A program may use at most 1 GiB of HBM per device.

```python
import jax
import jax.numpy as jnp
from jax import lax

BATCH = 4
SEQ = 512
D = 1024
VOCAB = 50280
NORM_EPS = 1e-5
HEAD_SCALE = 2.0
TOK_BLOCK = min(SEQ, 256)


def draw_targets(tgt_key):
    k_pick, k_head, k_wide = jax.random.split(tgt_key, 3)
    pick_wide = jax.random.randint(k_pick, (BATCH, SEQ), 0, 4)
    head_ids = jax.random.randint(k_head, (BATCH, SEQ), 0, VOCAB // 16)
    wide_ids = jax.random.randint(k_wide, (BATCH, SEQ), 0, VOCAB)
    targets = jnp.where(pick_wide == 0, wide_ids, head_ids)
    return targets.at[0, 0].set(VOCAB - 1).at[0, 1].set(0).astype(jnp.int32)


def setup_inputs(seed: int = 0) -> dict:
    root_key = jax.random.key(seed)
    k_hid, k_res, k_tgt, k_emb, k_norm = jax.random.split(root_key, 5)
    hidden = jax.random.normal(k_hid, (BATCH, SEQ, D), jnp.float32).astype(jnp.bfloat16)
    residual = jax.random.normal(k_res, (BATCH, SEQ, D), jnp.float32)
    targets = draw_targets(k_tgt)
    embedding = (jax.random.normal(k_emb, (VOCAB, D), jnp.float32) * (HEAD_SCALE * D ** -0.5)).astype(jnp.bfloat16)
    norm_w = 1.0 + 0.3 * jax.random.normal(k_norm, (D,), jnp.float32)
    return {'hidden': hidden, 'residual': residual, 'targets': targets, 'embedding': embedding, 'norm_w': norm_w}


def norm_apply(resid, norm_w):
    inv_rms = lax.rsqrt(jnp.mean(resid * resid, axis=-1, keepdims=True) + NORM_EPS)
    return resid * inv_rms * norm_w


def reference(hidden, residual, targets, embedding, norm_w):
    n_tok = BATCH * SEQ
    inv_n = 1.0 / n_tok
    n_blocks = n_tok // TOK_BLOCK
    resid_all = (residual + hidden.astype(jnp.float32)).reshape(n_blocks, TOK_BLOCK, D)
    tgt_all = targets.reshape(n_blocks, TOK_BLOCK)
    vocab_ids = jnp.arange(VOCAB, dtype=jnp.int32)

    def block_step(carry_acc, blk_inputs):
        grad_emb, grad_w, loss_sum = carry_acc
        resid_blk, tgt_blk = blk_inputs
        normed, norm_vjp = jax.vjp(norm_apply, resid_blk, norm_w)
        h_blk = normed.astype(jnp.bfloat16)
        logits = jnp.dot(h_blk, embedding.T, preferred_element_type=jnp.float32)
        row_max = jnp.max(logits, axis=-1, keepdims=True)
        exp_shift = jnp.exp(logits - row_max)
        sum_exp = jnp.sum(exp_shift, axis=-1, keepdims=True)
        is_target = vocab_ids[None, :] == tgt_blk[:, None]
        tgt_logit = jnp.sum(jnp.where(is_target, logits, 0.0), axis=-1)
        log_norm = row_max[:, 0] + jnp.log(sum_exp[:, 0])
        prob_rows = exp_shift / sum_exp
        dlogits = (jnp.where(is_target, prob_rows - 1.0, prob_rows) * inv_n).astype(jnp.bfloat16)
        grad_h = jnp.dot(dlogits, embedding, preferred_element_type=jnp.float32)
        grad_r, grad_wb = norm_vjp(grad_h)
        grad_emb = grad_emb + jnp.dot(dlogits.T, h_blk, preferred_element_type=jnp.float32)
        return (grad_emb, grad_w + grad_wb, loss_sum + jnp.sum(log_norm - tgt_logit)), grad_r

    init_acc = (jnp.zeros((VOCAB, D), jnp.float32), jnp.zeros((D,), jnp.float32), jnp.zeros((), jnp.float32))
    final_acc, grad_rows = lax.scan(block_step, init_acc, (resid_all, tgt_all))
    grad_emb, grad_w, loss_sum = final_acc
    return (loss_sum * inv_n, grad_rows.reshape(BATCH, SEQ, D), grad_emb, grad_w)
```

```python
import jax
import jax.numpy as jnp
from jax import lax
from jax.sharding import PartitionSpec as P

NORM_EPS = 1e-5


def solution(mesh):
    def program(hidden, residual, targets, embedding, norm_w):
        inv_n = 1.0 / (hidden.shape[0] * hidden.shape[1])

        def local_part(hid_loc, res_loc, tgt_loc, emb_loc, norm_vec):
            n_batch, n_seq, d_model = hid_loc.shape
            n_rows = n_batch * n_seq
            vocab_loc = emb_loc.shape[0]
            resid = (res_loc + hid_loc.astype(jnp.float32)).reshape(n_rows, d_model)
            inv_rms = lax.rsqrt(jnp.mean(resid * resid, axis=-1, keepdims=True) + NORM_EPS)
            scaled_r = resid * inv_rms
            scaled_all = lax.all_gather(scaled_r, 'dp', tiled=True)
            tgt_all = lax.all_gather(tgt_loc.reshape(n_rows), 'dp', tiled=True)
            h_act = (scaled_all * norm_vec).astype(jnp.bfloat16)
            logits = jnp.einsum('td,vd->tv', h_act, emb_loc, preferred_element_type=jnp.float32)
            part_max = jnp.max(logits, axis=-1, keepdims=True)
            local_ids = tgt_all - lax.axis_index('tp') * vocab_loc
            is_target = lax.broadcasted_iota(jnp.int32, (1, vocab_loc), 1) == local_ids[:, None]
            part_sum = jnp.sum(jnp.exp(logits - part_max), axis=-1, keepdims=True)
            part_tgt = jnp.sum(jnp.where(is_target, logits, 0.0), axis=-1, keepdims=True)
            parts = lax.all_gather(jnp.concatenate([part_max, part_sum, part_tgt], axis=-1), 'tp')
            row_max = jnp.max(parts[:, :, 0:1], axis=0)
            sum_exp = jnp.sum(parts[:, :, 1:2] * jnp.exp(parts[:, :, 0:1] - row_max), axis=0)
            tgt_logit = jnp.sum(parts[:, :, 2:3], axis=0)
            loss_mean = jnp.sum(row_max + jnp.log(sum_exp) - tgt_logit) * inv_n
            prob_rows = jnp.exp(logits - row_max) / sum_exp
            dlogits = (jnp.where(is_target, prob_rows - 1.0, prob_rows) * inv_n).astype(jnp.bfloat16)
            my_rows = lax.dynamic_slice_in_dim(dlogits, lax.axis_index('dp') * n_rows, n_rows, 0)
            grad_h = lax.psum(jnp.einsum('tv,vd->td', my_rows, emb_loc, preferred_element_type=jnp.float32), 'tp')
            grad_emb = jnp.einsum('tv,td->vd', dlogits, h_act, preferred_element_type=jnp.float32)
            grad_scaled = grad_h * norm_vec
            grad_r = inv_rms * (grad_scaled - scaled_r * jnp.mean(grad_scaled * scaled_r, axis=-1, keepdims=True))
            grad_w = lax.psum(jnp.sum(grad_h * scaled_r, axis=0), 'dp')
            return loss_mean, grad_r.reshape(n_batch, n_seq, d_model), grad_emb, grad_w

        sharded = jax.shard_map(
            local_part, mesh=mesh,
            in_specs=(P('dp', None, None), P('dp', None, None), P('dp', None), P('tp', None), P(None)),
            out_specs=(P(), P('dp', None, None), P('tp', None), P(None)),
            check_vma=False)
        return sharded(hidden, residual, targets, embedding, norm_w)

    return program
```

```python
import functools

import jax
import jax.numpy as jnp
from jax import lax
from jax.experimental import pallas as pl
from jax.experimental.pallas import tpu as pltpu
from jax.sharding import PartitionSpec as P

NORM_EPS = 1e-5
CH = 256
STEP = 7
PIECES = (8, 8, 8, 8, 8, 6, 3)
TAIL = 64
F32, BF16 = jnp.float32, jnp.bfloat16
NN = (((1,), (0,)), ((), ()))
NT = (((1,), (1,)), ((), ()))
TN = (((0,), (0,)), ((), ()))
VM = pl.BlockSpec(memory_space=pltpu.VMEM)
HB = pl.BlockSpec(memory_space=pl.ANY)


def dot(a, b, dims):
    return lax.dot_general(a, b, dims, preferred_element_type=F32)


def weights(logit, top, rate, hit, inv_n):
    return (jnp.exp(logit - top) * rate - jnp.where(hit, inv_n, 0.0)).astype(BF16)


def rows_of(n, width, base):
    return lax.broadcasted_iota(jnp.int32, (n, width), 0) + base


def stats_kernel(tail_rows, core_ref, emb_ref, tail_ref, ha_ref, hb_ref, tgt_ref, log_ref, logt_ref, stat_ref, top, total, hits):
    step, core = pl.program_id(0), core_ref[0]
    half = ha_ref.shape[0]

    @pl.when(step == 0)
    def _():
        top[...] = jnp.full_like(top, -jnp.inf)
        total[...] = jnp.zeros_like(total)
        hits[...] = jnp.zeros_like(hits)

    def fold(cols, logit, hit):
        split = logit.reshape(-1, 8, half)
        new = jnp.maximum(top[:, cols], jnp.max(split, axis=0))
        total[:, cols] = total[:, cols] * jnp.exp(top[:, cols] - new) + jnp.sum(jnp.exp(split - new[None]), axis=0)
        top[:, cols] = new
        hits[:, cols] += jnp.sum(jnp.where(hit, logit, 0.0).reshape(-1, 8, half), axis=0)

    for k in range(STEP):
        rows = pl.ds(k * CH, CH)
        for side, h_ref in ((0, ha_ref), (1, hb_ref)):
            cols = pl.ds(side * half, half)
            logit = dot(emb_ref[rows, :], h_ref[...], NT)
            log_ref[rows, cols] = logit
            want = tgt_ref[0:1, cols] - (step * STEP + k) * CH
            fold(cols, logit, rows_of(CH, half, 0) == want)

    @pl.when(step == pl.num_programs(0) - 1)
    def _():
        for side, h_ref in ((0, ha_ref), (1, hb_ref)):
            cols = pl.ds(side * half, half)
            ids = rows_of(TAIL, half, 0)
            live = jnp.logical_and(ids < tail_rows, core == 0)
            logit = jnp.where(live, dot(tail_ref[...], h_ref[...], NT), -jnp.inf)
            logt_ref[:, cols] = logit
            fold(cols, logit, jnp.logical_and(ids == tgt_ref[1:2, cols], live))
        peak = jnp.max(top[...], axis=0, keepdims=True)
        stat_ref[...] = jnp.zeros_like(stat_ref)
        stat_ref[0:1, :] = peak
        stat_ref[1:2, :] = jnp.sum(total[...] * jnp.exp(top[...] - peak), axis=0, keepdims=True)
        stat_ref[2:3, :] = jnp.sum(hits[...], axis=0, keepdims=True)


def dh_kernel(tail_rows, inv_n, core_ref, emb_ref, log_ref, tail_ref, logt_ref, row_ref, tgt_ref, da_ref, db_ref, g_ref, gt_ref):
    step, core = pl.program_id(0), core_ref[0]
    half = da_ref.shape[0]

    @pl.when(step == 0)
    def _():
        da_ref[...] = jnp.zeros_like(da_ref)
        db_ref[...] = jnp.zeros_like(db_ref)

    for k in range(STEP):
        rows = pl.ds(k * CH, CH)
        for side, d_ref in ((0, da_ref), (1, db_ref)):
            cols = pl.ds(side * half, half)
            want = tgt_ref[0:1, cols] - (step * STEP + k) * CH
            g_ref[rows, cols] = weights(log_ref[rows, cols], row_ref[0:1, cols], row_ref[1:2, cols], rows_of(CH, half, 0) == want, inv_n)
            d_ref[...] += dot(g_ref[rows, cols], emb_ref[rows, :], TN)

    @pl.when(step == pl.num_programs(0) - 1)
    def _():
        for side, d_ref in ((0, da_ref), (1, db_ref)):
            cols = pl.ds(side * half, half)
            ids = rows_of(TAIL, half, 0)
            live = jnp.logical_and(ids < tail_rows, core == 0)
            hit = jnp.logical_and(ids == tgt_ref[1:2, cols], live)
            gt_ref[:, cols] = weights(logt_ref[:, cols], row_ref[0:1, cols], row_ref[1:2, cols], hit, inv_n)
            d_ref[...] += dot(gt_ref[:, cols], tail_ref[...], TN)


def grad_kernel(first, count, late, inv_n, core_ref, emb_ref, log_ref, ha_ref, hb_ref, hc_ref, hd_ref, row_ref, rowx_ref, tgt_ref, tgtx_ref, *refs):
    per_core = sum(PIECES)
    refs = list(refs)
    if first:
        refs.pop(0)
    got_ref = refs.pop(0) if late else None
    out_ref, piece_ref, ga_ref, gx_ref, lx_ref, own_sem, got_sem = refs
    step, core = pl.program_id(0), core_ref[0]
    half = ha_ref.shape[0]
    rows = pl.ds(pl.multiple_of(step * CH, CH), CH)

    def own_copy(k):
        place = pl.multiple_of((core * per_core + first + k) * CH, CH)
        return pltpu.make_async_copy(piece_ref.at[pl.ds(pl.multiple_of(k * CH, CH), CH)], out_ref.at[pl.ds(place, CH)], own_sem)

    if late:
        back, size = late
        place = pl.multiple_of(((1 - core) * per_core + back) * CH, CH)
        got_copy = pltpu.make_async_copy(got_ref, out_ref.at[pl.ds(place, size * CH)], got_sem)

        @pl.when(step == 0)
        def _():
            got_copy.start()

    base = (first + step) * CH
    for side in (0, 1):
        cols = pl.ds(side * half, half)
        want = tgt_ref[0:1, cols] - base
        ga_ref[:, cols] = weights(log_ref[:, cols], row_ref[0:1, cols], row_ref[1:2, cols], rows_of(CH, half, 0) == want, inv_n)
    for side, h_ref in ((0, hc_ref), (1, hd_ref)):
        cols = pl.ds(side * half, half)
        lx_ref[:, cols] = dot(emb_ref[...], h_ref[...], NT)
    piece_ref[rows, :] = dot(ga_ref[:, pl.ds(0, half)], ha_ref[...], NN) + dot(ga_ref[:, pl.ds(half, half)], hb_ref[...], NN)
    for side in (0, 1):
        cols = pl.ds(side * half, half)
        want = tgtx_ref[0:1, cols] - base
        gx_ref[:, cols] = weights(lx_ref[:, cols], rowx_ref[0:1, cols], rowx_ref[1:2, cols], rows_of(CH, half, 0) == want, inv_n)
    piece_ref[rows, :] += dot(gx_ref[:, pl.ds(0, half)], hc_ref[...], NN) + dot(gx_ref[:, pl.ds(half, half)], hd_ref[...], NN)
    own_copy(step).start()

    @pl.when(step == count - 1)
    def _():
        def drain(k, _):
            own_copy(k).wait()
            return 0

        lax.fori_loop(0, count, drain, 0)
        if late:
            got_copy.wait()


def tail_kernel(inv_n, core_ref, tail_ref, ha_ref, hb_ref, hc_ref, hd_ref, row_ref, rowx_ref, tgt_ref, tgtx_ref, _, out_ref, g_ref):
    half = ha_ref.shape[0]
    grad = jnp.zeros(out_ref.shape, F32)
    ids = rows_of(TAIL, half, 0)
    for h_ref, r_ref, t_ref, side in ((ha_ref, row_ref, tgt_ref, 0), (hb_ref, row_ref, tgt_ref, 1), (hc_ref, rowx_ref, tgtx_ref, 0), (hd_ref, rowx_ref, tgtx_ref, 1)):
        cols = pl.ds(side * half, half)
        logit = dot(tail_ref[...], h_ref[...], NT)
        g_ref[...] = weights(logit, r_ref[0:1, cols], r_ref[1:2, cols], ids == t_ref[1:2, cols], inv_n)
        grad += dot(g_ref[...], h_ref[...], NN)
    out_ref[...] = grad


def last_kernel(late, core_ref, _, got_ref, out_ref, got_sem):
    back, size = late
    place = pl.multiple_of(((1 - core_ref[0]) * sum(PIECES) + back) * CH, CH)
    copy = pltpu.make_async_copy(got_ref, out_ref.at[pl.ds(place, size * CH)], got_sem)
    copy.start()
    copy.wait()


def cost(flops, moved):
    return pl.CostEstimate(flops=int(flops), bytes_accessed=int(moved), transcendentals=0)


def params(mib):
    return pltpu.CompilerParams(vmem_limit_bytes=mib << 20)


def solution(mesh):
    n_tp, n_dp = mesh.shape['tp'], mesh.shape['dp']

    def program(hidden, residual, targets, embedding, norm_w):
        inv_n = 1.0 / (hidden.shape[0] * hidden.shape[1])

        def local_part(hid_loc, res_loc, tgt_loc, emb_loc, norm_vec):
            n_batch, n_seq, d = hid_loc.shape
            half = n_batch * n_seq
            vocab_loc = emb_loc.shape[0]
            per_core = sum(PIECES)
            tail_rows = vocab_loc - 2 * per_core * CH
            my_tp, my_dp = lax.axis_index('tp'), lax.axis_index('dp')
            core = lax.rem(my_dp, 2)
            core_arg = core.reshape(1)
            swap = [(i, i ^ 1) for i in range(n_dp)]
            cross = [(i, i ^ 2) for i in range(n_dp)]
            flip = [(i, i ^ 1) for i in range(n_tp)]
            flip_swap = [(t * n_dp + i, (t ^ 1) * n_dp + (i ^ 1)) for t in range(n_tp) for i in range(n_dp)]

            resid = (res_loc + hid_loc.astype(F32)).reshape(half, d)
            inv_rms = lax.rsqrt(jnp.mean(resid * resid, axis=-1, keepdims=True) + NORM_EPS)
            scaled = resid * inv_rms
            tgt_own = tgt_loc.reshape(1, half)

            def act(n):
                return (n * norm_vec).astype(BF16)

            scaled_sib = lax.ppermute(scaled, 'dp', swap)
            tgt_sib = lax.ppermute(tgt_own, 'dp', swap)
            scaled_far = lax.ppermute(scaled, 'dp', cross)
            ha, hb = act(scaled), act(scaled_sib)

            def relative(both):
                shifted = both - my_tp * vocab_loc
                rel = jnp.concatenate([shifted - core * (per_core * CH), shifted - 2 * per_core * CH], axis=0)
                return jnp.pad(rel, ((0, 6), (0, 0)))

            tgt_raw = jnp.concatenate([tgt_own, tgt_sib], axis=1)
            tgt_near = relative(tgt_raw)
            tgt_far = relative(lax.ppermute(tgt_raw, 'dp', cross))
            emb_tail = jnp.pad(emb_loc[2 * per_core * CH:], ((0, TAIL - tail_rows), (0, 0)))

            steps, blk = per_core // STEP, STEP * CH
            flops_unit = 2.0 * CH * d * half
            smem = pltpu.SMEM
            logits, logits_tail, stat = pl.pallas_call(
                functools.partial(stats_kernel, tail_rows),
                grid_spec=pltpu.PrefetchScalarGridSpec(
                    num_scalar_prefetch=1, grid=(steps,),
                    in_specs=[pl.BlockSpec((blk, d), lambda i, c: (c[0] * steps + i, 0)), VM, VM, VM, VM],
                    out_specs=[pl.BlockSpec((blk, 2 * half), lambda i, c: (i, 0)), VM, VM],
                    scratch_shapes=[pltpu.VMEM((8, 2 * half), F32)] * 3),
                out_shape=[jax.ShapeDtypeStruct((per_core * CH, 2 * half), F32),
                           jax.ShapeDtypeStruct((TAIL, 2 * half), F32), jax.ShapeDtypeStruct((8, 2 * half), F32)],
                compiler_params=params(44),
                cost_estimate=cost(flops_unit * per_core * 2, per_core * CH * (2 * d + 8 * half)),
            )(core_arg, emb_loc, emb_tail, ha, hb, tgt_near)

            def turned(x):
                return jnp.concatenate([x[:, half:], x[:, :half]], axis=1)

            near = stat[0:3]
            sib = turned(lax.ppermute(near, 'dp', swap))
            over = lax.ppermute(near, 'tp', flip)
            over_sib = turned(lax.ppermute(near, ('tp', 'dp'), flip_swap))
            top = jnp.maximum(jnp.maximum(near[0], sib[0]), jnp.maximum(over[0], over_sib[0]))
            parts = [p[1] * jnp.exp(p[0] - top) for p in (near, sib, over, over_sib)]
            sum_exp = (parts[0] + parts[1]) + (parts[2] + parts[3])
            tgt_logit = (near[2] + sib[2]) + (over[2] + over_sib[2])
            token_loss = top + jnp.log(sum_exp) - tgt_logit
            row_near = jnp.pad(jnp.stack([top, inv_n / sum_exp]), ((0, 6), (0, 0)))
            row_near, scaled_far = lax.optimization_barrier((row_near, scaled_far))
            scaled_far_sib = lax.ppermute(scaled_far, 'dp', swap)
            row_far = lax.ppermute(row_near, 'dp', cross)
            loss_chip = jnp.sum(token_loss[:half]) + jnp.sum(token_loss[half:])
            loss_mean = (loss_chip + lax.ppermute(loss_chip.reshape(1), 'dp', cross)[0]) * inv_n

            dh_own, dh_sib = pl.pallas_call(
                functools.partial(dh_kernel, tail_rows, inv_n),
                grid_spec=pltpu.PrefetchScalarGridSpec(
                    num_scalar_prefetch=1, grid=(steps,),
                    in_specs=[pl.BlockSpec((blk, d), lambda i, c: (c[0] * steps + i, 0)),
                              pl.BlockSpec((blk, 2 * half), lambda i, c: (i, 0)), VM, VM, VM, VM],
                    out_specs=[VM, VM],
                    scratch_shapes=[pltpu.VMEM((blk, 2 * half), BF16), pltpu.VMEM((TAIL, 2 * half), BF16)]),
                out_shape=[jax.ShapeDtypeStruct((half, d), F32)] * 2,
                compiler_params=params(44),
                cost_estimate=cost(flops_unit * per_core * 2, per_core * CH * (2 * d + 8 * half)),
            )(core_arg, emb_loc, logits, emb_tail, logits_tail, row_near, tgt_near)

            row_near, row_far, scaled_far, scaled_far_sib, dh_own, dh_sib = lax.optimization_barrier(
                (row_near, row_far, scaled_far, scaled_far_sib, dh_own, dh_sib))
            hc, hd = act(scaled_far), act(scaled_far_sib)
            dh_chip = dh_own + lax.ppermute(dh_sib, 'dp', swap)
            grad_h = dh_chip + lax.ppermute(dh_chip, 'tp', flip)
            grad_scaled = grad_h * norm_vec
            grad_r = inv_rms * (grad_scaled - scaled * jnp.mean(grad_scaled * scaled, axis=-1, keepdims=True))
            grad_w = jnp.sum(grad_h * scaled, axis=0, keepdims=True)
            grad_w = grad_w + lax.ppermute(grad_w, 'dp', swap)
            grad_w = (grad_w + lax.ppermute(grad_w, 'dp', cross)).reshape(d)

            def piece_call(first, count, out, late, got):
                extra = ([] if out is None else [out]) + ([] if got is None else [got])
                kern = functools.partial(grad_kernel, first, count, late, inv_n)
                return pl.pallas_call(
                    kern,
                    grid_spec=pltpu.PrefetchScalarGridSpec(
                        num_scalar_prefetch=1, grid=(count,),
                        in_specs=[pl.BlockSpec((CH, d), lambda i, c: (c[0] * per_core + first + i, 0)),
                                  pl.BlockSpec((CH, 2 * half), lambda i, c: (first + i, 0))] + [VM] * 8
                        + ([] if out is None else [HB]) + ([] if got is None else [VM]),
                        out_specs=[HB, VM],
                        scratch_shapes=[pltpu.VMEM((CH, 2 * half), BF16), pltpu.VMEM((CH, 2 * half), BF16), pltpu.VMEM((CH, 2 * half), F32),
                                        pltpu.SemaphoreType.DMA, pltpu.SemaphoreType.DMA]),
                    out_shape=[jax.ShapeDtypeStruct((vocab_loc, d), F32), jax.ShapeDtypeStruct((count * CH, d), F32)],
                    input_output_aliases={} if out is None else {11: 0},
                    compiler_params=params(14),
                    cost_estimate=cost(flops_unit * count * 6, count * CH * (2 * d + 8 * half + 8 * d)),
                )(core_arg, emb_loc, logits, ha, hb, hc, hd, row_near, row_far, tgt_near, tgt_far, *extra)

            out, first, arrived = None, 0, []
            for k, count in enumerate(PIECES):
                late, got = arrived[k - 2] if k >= 2 else (None, None)
                out, piece = piece_call(first, count, out, late, got)
                arrived.append(((first, count), lax.ppermute(piece, 'dp', swap)))
                first += count

            out = pl.pallas_call(
                functools.partial(tail_kernel, inv_n),
                grid_spec=pltpu.PrefetchScalarGridSpec(
                    num_scalar_prefetch=1, grid=(1,), in_specs=[VM] * 9 + [HB],
                    out_specs=pl.BlockSpec((TAIL, d), lambda i, c: (2 * per_core * CH // TAIL, 0)),
                    scratch_shapes=[pltpu.VMEM((TAIL, half), BF16)]),
                out_shape=jax.ShapeDtypeStruct((vocab_loc, d), F32),
                input_output_aliases={10: 0},
                compiler_params=params(14),
                cost_estimate=cost(2.0 * TAIL * d * half * 8, 4 * TAIL * d),
            )(core_arg, emb_tail, ha, hb, hc, hd, row_near, row_far, tgt_near, tgt_far, out)
            for late, got in arrived[-2:]:
                out = pl.pallas_call(
                    functools.partial(last_kernel, late),
                    grid_spec=pltpu.PrefetchScalarGridSpec(
                        num_scalar_prefetch=1, grid=(1,), in_specs=[HB, VM], out_specs=HB, scratch_shapes=[pltpu.SemaphoreType.DMA]),
                    out_shape=jax.ShapeDtypeStruct((vocab_loc, d), F32),
                    input_output_aliases={1: 0},
                    compiler_params=params(14),
                    cost_estimate=cost(1e6, 4 * late[1] * CH * d),
                )(core_arg, out, got)
            return loss_mean, grad_r.reshape(n_batch, n_seq, d), out, grad_w

        sharded = jax.shard_map(
            local_part, mesh=mesh,
            in_specs=(P('dp', None, None), P('dp', None, None), P('dp', None), P('tp', None), P(None)),
            out_specs=(P(), P('dp', None, None), P('tp', None), P(None)),
            check_vma=False)
        return sharded(hidden, residual, targets, embedding, norm_w)

    return program
```

```python
import functools

import jax
import jax.numpy as jnp
from jax import lax
from jax.experimental import pallas as pl
from jax.experimental.pallas import tpu as pltpu
from jax.sharding import PartitionSpec as P


NORM_EPS = 1e-5
CH = 256
STEP = 7
PIECES = (5, 5, 5, 5, 5, 5, 5, 5, 4, 3, 2)
TAIL = 64
F32, BF16 = jnp.float32, jnp.bfloat16
NN = (((1,), (0,)), ((), ()))
NT = (((1,), (1,)), ((), ()))
TN = (((0,), (0,)), ((), ()))
VM = pl.BlockSpec(memory_space=pltpu.VMEM)
HB = pl.BlockSpec(memory_space=pl.ANY)


def dot(a, b, dims):
    return lax.dot_general(a, b, dims, preferred_element_type=F32)


def weights(logit, top, rate, hit, inv_n):
    return (jnp.exp(logit - top) * rate - jnp.where(hit, inv_n, 0.0)).astype(BF16)


def rows_of(n, width, base):
    return lax.broadcasted_iota(jnp.int32, (n, width), 0) + base


def stats_kernel(tail_rows, core_ref, emb_ref, tail_ref, ha_ref, hb_ref, tgt_ref, log_ref, logt_ref, stat_ref, top, total, hits):
    step, core = pl.program_id(0), core_ref[0]
    half = ha_ref.shape[0]

    @pl.when(step == 0)
    def _():
        top[...] = jnp.full_like(top, -jnp.inf)
        total[...] = jnp.zeros_like(total)
        hits[...] = jnp.zeros_like(hits)

    def fold(cols, logit, hit):
        split = logit.reshape(-1, 8, half)
        new = jnp.maximum(top[:, cols], jnp.max(split, axis=0))
        total[:, cols] = total[:, cols] * jnp.exp(top[:, cols] - new) + jnp.sum(jnp.exp(split - new[None]), axis=0)
        top[:, cols] = new
        hits[:, cols] += jnp.sum(jnp.where(hit, logit, 0.0).reshape(-1, 8, half), axis=0)

    for k in range(STEP):
        rows = pl.ds(k * CH, CH)
        for side, h_ref in ((0, ha_ref), (1, hb_ref)):
            cols = pl.ds(side * half, half)
            logit = dot(emb_ref[rows, :], h_ref[...], NT)
            log_ref[rows, cols] = logit
            want = tgt_ref[0:1, cols] - (step * STEP + k) * CH
            fold(cols, logit, rows_of(CH, half, 0) == want)

    @pl.when(step == pl.num_programs(0) - 1)
    def _():
        for side, h_ref in ((0, ha_ref), (1, hb_ref)):
            cols = pl.ds(side * half, half)
            ids = rows_of(TAIL, half, 0)
            live = jnp.logical_and(ids < tail_rows, core == 0)
            logit = jnp.where(live, dot(tail_ref[...], h_ref[...], NT), -jnp.inf)
            logt_ref[:, cols] = logit
            fold(cols, logit, jnp.logical_and(ids == tgt_ref[1:2, cols], live))
        peak = jnp.max(top[...], axis=0, keepdims=True)
        stat_ref[...] = jnp.zeros_like(stat_ref)
        stat_ref[0:1, :] = peak
        stat_ref[1:2, :] = jnp.sum(total[...] * jnp.exp(top[...] - peak), axis=0, keepdims=True)
        stat_ref[2:3, :] = jnp.sum(hits[...], axis=0, keepdims=True)


def dh_kernel(tail_rows, inv_n, core_ref, emb_ref, log_ref, tail_ref, logt_ref, row_ref, tgt_ref, da_ref, db_ref, loss_ref, g_ref, gt_ref):
    step, core = pl.program_id(0), core_ref[0]
    half = da_ref.shape[0]

    @pl.when(step == 0)
    def _():
        loss_ref[...] = jnp.full(loss_ref.shape, jnp.sum(row_ref[2:3, pl.ds(0, half)]) + jnp.sum(row_ref[2:3, pl.ds(half, half)]))
        da_ref[...] = jnp.zeros_like(da_ref)
        db_ref[...] = jnp.zeros_like(db_ref)

    for k in range(STEP):
        rows = pl.ds(k * CH, CH)
        for side, d_ref in ((0, da_ref), (1, db_ref)):
            cols = pl.ds(side * half, half)
            want = tgt_ref[0:1, cols] - (step * STEP + k) * CH
            g_ref[rows, cols] = weights(log_ref[rows, cols], row_ref[0:1, cols], row_ref[1:2, cols], rows_of(CH, half, 0) == want, inv_n)
            d_ref[...] += dot(g_ref[rows, cols], emb_ref[rows, :], TN)

    @pl.when(step == pl.num_programs(0) - 1)
    def _():
        for side, d_ref in ((0, da_ref), (1, db_ref)):
            cols = pl.ds(side * half, half)
            ids = rows_of(TAIL, half, 0)
            live = jnp.logical_and(ids < tail_rows, core == 0)
            hit = jnp.logical_and(ids == tgt_ref[1:2, cols], live)
            gt_ref[:, cols] = weights(logt_ref[:, cols], row_ref[0:1, cols], row_ref[1:2, cols], hit, inv_n)
            d_ref[...] += dot(gt_ref[:, cols], tail_ref[...], TN)


def rows_at(core, first, count):
    return pl.ds(pl.multiple_of((core * sum(PIECES) + first) * CH, CH), count * CH)


def grad_kernel(first, count, prev, late, inv_n, core_ref, emb_ref, log_ref, ha_ref, hb_ref, hc_ref, hd_ref, row_ref, rowx_ref, tgt_ref, tgtx_ref, mark_ref, *refs):
    per_core = sum(PIECES)
    refs = list(refs)
    if prev:
        refs = refs[3:]
    own_ref = refs.pop(0) if prev else None
    got_ref = refs.pop(0) if late else None
    out_ref, emb_buf, log_buf, piece_ref, token_ref, ga_ref, gx_ref, lx_ref, emb_sem, log_sem, own_sem, got_sem = refs
    core = core_ref[0]
    half = ha_ref.shape[0]
    token_ref[...] = mark_ref[...]

    def fetch(k):
        slot = lax.rem(k, 2)
        mine = pl.ds(pl.multiple_of(k * CH, CH), CH)
        return (pltpu.make_async_copy(emb_ref.at[rows_at(core, k, 1)], emb_buf.at[slot], emb_sem),
                pltpu.make_async_copy(log_ref.at[mine], log_buf.at[slot], log_sem))

    writes = []
    if prev:
        writes.append(pltpu.make_async_copy(own_ref, out_ref.at[rows_at(core, *prev)], own_sem))
    if late:
        writes.append(pltpu.make_async_copy(got_ref, out_ref.at[rows_at(1 - core, *late)], got_sem))
    if not prev:
        for copy in fetch(jnp.int32(first)):
            copy.start()
        for copy in fetch(jnp.int32(first)):
            copy.wait()
    for copy in writes:
        copy.start()

    def step(i, carry):
        k = first + i
        slot = lax.rem(k, 2)
        rows = pl.ds(pl.multiple_of(i * CH, CH), CH)
        more = k + 1 < per_core

        @pl.when(more)
        def _():
            for copy in fetch(k + 1):
                copy.start()

        base = k * CH
        for side in (0, 1):
            cols = pl.ds(side * half, half)
            want = tgt_ref[0:1, cols] - base
            ga_ref[:, cols] = weights(log_buf[slot, :, cols], row_ref[0:1, cols], row_ref[1:2, cols], rows_of(CH, half, 0) == want, inv_n)
        for side, h_ref in ((0, hc_ref), (1, hd_ref)):
            cols = pl.ds(side * half, half)
            lx_ref[:, cols] = dot(emb_buf[slot], h_ref[...], NT)
        piece_ref[rows, :] = dot(ga_ref[:, pl.ds(0, half)], ha_ref[...], NN) + dot(ga_ref[:, pl.ds(half, half)], hb_ref[...], NN)
        for side in (0, 1):
            cols = pl.ds(side * half, half)
            want = tgtx_ref[0:1, cols] - base
            gx_ref[:, cols] = weights(lx_ref[:, cols], rowx_ref[0:1, cols], rowx_ref[1:2, cols], rows_of(CH, half, 0) == want, inv_n)
        piece_ref[rows, :] += dot(gx_ref[:, pl.ds(0, half)], hc_ref[...], NN) + dot(gx_ref[:, pl.ds(half, half)], hd_ref[...], NN)

        @pl.when(more)
        def _():
            for copy in fetch(k + 1):
                copy.wait()

        return carry

    lax.fori_loop(0, count, step, 0)
    for copy in writes:
        copy.wait()


def tail_kernel(inv_n, core_ref, tail_ref, ha_ref, hb_ref, hc_ref, hd_ref, row_ref, rowx_ref, tgt_ref, tgtx_ref, _, out_ref, g_ref):
    half = ha_ref.shape[0]
    grad = jnp.zeros(out_ref.shape, F32)
    ids = rows_of(TAIL, half, 0)
    for h_ref, r_ref, t_ref, side in ((ha_ref, row_ref, tgt_ref, 0), (hb_ref, row_ref, tgt_ref, 1), (hc_ref, rowx_ref, tgtx_ref, 0), (hd_ref, rowx_ref, tgtx_ref, 1)):
        cols = pl.ds(side * half, half)
        logit = dot(tail_ref[...], h_ref[...], NT)
        g_ref[...] = weights(logit, r_ref[0:1, cols], r_ref[1:2, cols], ids == t_ref[1:2, cols], inv_n)
        grad += dot(g_ref[...], h_ref[...], NN)
    out_ref[...] = grad


def last_kernel(places, core_ref, _, *refs):
    srcs, out_ref, sems = refs[:len(places)], refs[len(places)], refs[len(places) + 1:]
    copies = []
    for src, sem, (other, place) in zip(srcs, sems, places):
        side = 1 - core_ref[0] if other else core_ref[0]
        copies.append(pltpu.make_async_copy(src, out_ref.at[rows_at(side, *place)], sem))
    for copy in copies:
        copy.start()
    for copy in copies:
        copy.wait()


def cost(flops, moved):
    return pl.CostEstimate(flops=int(flops), bytes_accessed=int(moved), transcendentals=0)


def params(mib):
    return pltpu.CompilerParams(vmem_limit_bytes=mib << 20)


def solution(mesh):
    n_tp, n_dp = mesh.shape['tp'], mesh.shape['dp']

    def program(hidden, residual, targets, embedding, norm_w):
        inv_n = 1.0 / (hidden.shape[0] * hidden.shape[1])

        def local_part(hid_loc, res_loc, tgt_loc, emb_loc, norm_vec):
            n_batch, n_seq, d = hid_loc.shape
            half = n_batch * n_seq
            vocab_loc = emb_loc.shape[0]
            per_core = sum(PIECES)
            tail_rows = vocab_loc - 2 * per_core * CH
            my_tp, my_dp = lax.axis_index('tp'), lax.axis_index('dp')
            core = lax.rem(my_dp, 2)
            core_arg = core.reshape(1)
            swap = [(i, i ^ 1) for i in range(n_dp)]
            cross = [(i, i ^ 2) for i in range(n_dp)]
            flip = [(i, i ^ 1) for i in range(n_tp)]
            flip_swap = [(t * n_dp + i, (t ^ 1) * n_dp + (i ^ 1)) for t in range(n_tp) for i in range(n_dp)]

            resid = (res_loc + hid_loc.astype(F32)).reshape(half, d)
            inv_rms = lax.rsqrt(jnp.mean(resid * resid, axis=-1, keepdims=True) + NORM_EPS)
            scaled = resid * inv_rms
            tgt_own = tgt_loc.reshape(1, half)

            def act(n):
                return (n * norm_vec).astype(BF16)

            scaled_sib = lax.ppermute(scaled, 'dp', swap)
            tgt_sib = lax.ppermute(tgt_own, 'dp', swap)
            scaled_far = lax.ppermute(scaled, 'dp', cross)
            ha, hb = act(scaled), act(scaled_sib)

            def relative(both):
                shifted = both - my_tp * vocab_loc
                rel = jnp.concatenate([shifted - core * (per_core * CH), shifted - 2 * per_core * CH], axis=0)
                return jnp.pad(rel, ((0, 6), (0, 0)))

            tgt_raw = jnp.concatenate([tgt_own, tgt_sib], axis=1)
            tgt_near = relative(tgt_raw)
            tgt_raw_far = lax.ppermute(tgt_raw, 'dp', cross)
            emb_tail = jnp.pad(emb_loc[2 * per_core * CH:], ((0, TAIL - tail_rows), (0, 0)))

            steps, blk = per_core // STEP, STEP * CH
            flops_unit = 2.0 * CH * d * half
            logits, logits_tail, stat = pl.pallas_call(
                functools.partial(stats_kernel, tail_rows),
                grid_spec=pltpu.PrefetchScalarGridSpec(
                    num_scalar_prefetch=1, grid=(steps,),
                    in_specs=[pl.BlockSpec((blk, d), lambda i, c: (c[0] * steps + i, 0)), VM, VM, VM, VM],
                    out_specs=[pl.BlockSpec((blk, 2 * half), lambda i, c: (i, 0)), VM, VM],
                    scratch_shapes=[pltpu.VMEM((8, 2 * half), F32)] * 3),
                out_shape=[jax.ShapeDtypeStruct((per_core * CH, 2 * half), F32),
                           jax.ShapeDtypeStruct((TAIL, 2 * half), F32), jax.ShapeDtypeStruct((8, 2 * half), F32)],
                compiler_params=params(27),
                cost_estimate=cost(flops_unit * per_core * 2, per_core * CH * (2 * d + 8 * half)),
            )(core_arg, emb_loc, emb_tail, ha, hb, tgt_near)

            def turned(x):
                return jnp.concatenate([x[:, half:], x[:, :half]], axis=1)

            near = stat[0:3]
            sib = turned(lax.ppermute(near, 'dp', swap))
            over = lax.ppermute(near, 'tp', flip)
            over_sib = turned(lax.ppermute(near, ('tp', 'dp'), flip_swap))
            top = jnp.maximum(jnp.maximum(near[0], sib[0]), jnp.maximum(over[0], over_sib[0]))
            parts = [p[1] * jnp.exp(p[0] - top) for p in (near, sib, over, over_sib)]
            sum_exp = (parts[0] + parts[1]) + (parts[2] + parts[3])
            tgt_logit = (near[2] + sib[2]) + (over[2] + over_sib[2])
            token_loss = top + jnp.log(sum_exp) - tgt_logit
            row_near = jnp.pad(jnp.stack([top, inv_n / sum_exp, token_loss]), ((0, 5), (0, 0)))
            row_near, scaled_far, tgt_raw_far = lax.optimization_barrier((row_near, scaled_far, tgt_raw_far))
            tgt_far = relative(tgt_raw_far)
            scaled_far_sib = lax.ppermute(scaled_far, 'dp', swap)
            row_far = lax.ppermute(row_near, 'dp', cross)

            dh_own, dh_sib, loss_chip = pl.pallas_call(
                functools.partial(dh_kernel, tail_rows, inv_n),
                grid_spec=pltpu.PrefetchScalarGridSpec(
                    num_scalar_prefetch=1, grid=(steps,),
                    in_specs=[pl.BlockSpec((blk, d), lambda i, c: (c[0] * steps + i, 0)),
                              pl.BlockSpec((blk, 2 * half), lambda i, c: (i, 0)), VM, VM, VM, VM],
                    out_specs=[VM, VM, VM],
                    scratch_shapes=[pltpu.VMEM((blk, 2 * half), BF16), pltpu.VMEM((TAIL, 2 * half), BF16)]),
                out_shape=[jax.ShapeDtypeStruct((half, d), F32)] * 2 + [jax.ShapeDtypeStruct((8, 128), F32)],
                compiler_params=params(31),
                cost_estimate=cost(flops_unit * per_core * 2, per_core * CH * (2 * d + 8 * half)),
            )(core_arg, emb_loc, logits, emb_tail, logits_tail, row_near, tgt_near)

            tie = lax.optimization_barrier
            row_near, row_far, scaled_far, scaled_far_sib, dh_own, dh_sib, tgt_far = tie(
                (row_near, row_far, scaled_far, scaled_far_sib, dh_own, dh_sib, tgt_far))
            hc, hd = act(scaled_far), act(scaled_far_sib)
            dh_got = lax.ppermute(dh_sib, 'dp', swap)
            loss_far = lax.ppermute(loss_chip, 'dp', cross)

            def piece_call(first, count, mark, out, bufs, prev, own, late, got):
                extra = ([] if out is None else [out, *bufs, own]) + ([] if got is None else [got])
                specs = ([] if out is None else [HB, VM, VM, VM]) + ([] if got is None else [VM])
                return pl.pallas_call(
                    functools.partial(grad_kernel, first, count, prev, late, inv_n),
                    in_specs=[pl.BlockSpec(memory_space=pltpu.SMEM), HB, HB] + [VM] * 9 + specs,
                    out_specs=[HB, VM, VM, VM, VM],
                    scratch_shapes=[pltpu.VMEM((CH, 2 * half), BF16), pltpu.VMEM((CH, 2 * half), BF16), pltpu.VMEM((CH, 2 * half), F32)]
                    + [pltpu.SemaphoreType.DMA] * 4,
                    out_shape=[jax.ShapeDtypeStruct((vocab_loc, d), F32), jax.ShapeDtypeStruct((2, CH, d), BF16),
                               jax.ShapeDtypeStruct((2, CH, 2 * half), F32), pltpu.VMEM((count * CH, d), F32),
                               jax.ShapeDtypeStruct((8, 128), F32)],
                    input_output_aliases={} if out is None else {12: 0, 13: 1, 14: 2},
                    compiler_params=params(10),
                    cost_estimate=cost(flops_unit * count * 6, count * CH * (2 * d + 8 * half + 8 * d)),
                )(core_arg, emb_loc, logits, ha, hb, hc, hd, row_near, row_far, tgt_near, tgt_far, mark, *extra)

            out, bufs, first, own, prev, arrived = None, (), 0, None, None, []
            mark = jnp.zeros((8, 128), F32)
            for k, count in enumerate(PIECES):
                late, got = arrived[k - 2] if k >= 2 else (None, None)
                out, *bufs, piece, mark = piece_call(first, count, mark, out, bufs, prev, own, late, got)
                own, prev = piece, (first, count)
                arrived.append((prev, lax.ppermute(piece, 'dp', swap)))
                first += count
                if k == 0:
                    dh_got, loss_far, mark = tie((dh_got, loss_far, mark))
                    dh_chip, mark = tie((dh_own + dh_got, mark))
                    dh_far = lax.ppermute(dh_chip, 'tp', flip)
                if k == 4:
                    dh_far, mark = tie((dh_far, mark))
                    grad_h = dh_chip + dh_far
                    grad_scaled = grad_h * norm_vec
                    grad_r = inv_rms * (grad_scaled - scaled * jnp.mean(grad_scaled * scaled, axis=-1, keepdims=True))
                    grad_w = jnp.sum(grad_h * scaled, axis=0, keepdims=True)
                    grad_r, grad_w, mark = tie((grad_r, grad_w, mark))
                    grad_w_got = lax.ppermute(grad_w, 'dp', swap)
                if k == 5:
                    grad_w_got, mark = tie((grad_w_got, mark))
                    grad_w, mark = tie((grad_w + grad_w_got, mark))
                    grad_w_got = lax.ppermute(grad_w, 'dp', cross)
            loss_mean = ((loss_chip + loss_far) * inv_n)[0, 0]
            grad_w = (grad_w + grad_w_got).reshape(d)

            out = pl.pallas_call(
                functools.partial(tail_kernel, inv_n),
                grid_spec=pltpu.PrefetchScalarGridSpec(
                    num_scalar_prefetch=1, grid=(1,), in_specs=[VM] * 9 + [HB],
                    out_specs=pl.BlockSpec((TAIL, d), lambda i, c: (2 * per_core * CH // TAIL, 0)),
                    scratch_shapes=[pltpu.VMEM((TAIL, half), BF16)]),
                out_shape=jax.ShapeDtypeStruct((vocab_loc, d), F32),
                input_output_aliases={10: 0},
                compiler_params=params(14),
                cost_estimate=cost(2.0 * TAIL * d * half * 8, 4 * TAIL * d),
            )(core_arg, emb_tail, ha, hb, hc, hd, row_near, row_far, tgt_near, tgt_far, out)
            for parts in ([(False, prev, own), (True, *arrived[-2])], [(True, *arrived[-1])]):
                out = pl.pallas_call(
                    functools.partial(last_kernel, [p[:2] for p in parts]),
                    in_specs=[pl.BlockSpec(memory_space=pltpu.SMEM), HB] + [VM] * len(parts), out_specs=HB,
                    scratch_shapes=[pltpu.SemaphoreType.DMA] * len(parts),
                    out_shape=jax.ShapeDtypeStruct((vocab_loc, d), F32),
                    input_output_aliases={1: 0},
                    compiler_params=params(8),
                    cost_estimate=cost(1e6, sum(4 * p[1][1] * CH * d for p in parts)),
                )(core_arg, out, *[p[2] for p in parts])
            return loss_mean, grad_r.reshape(n_batch, n_seq, d), out, grad_w

        sharded = jax.shard_map(
            local_part, mesh=mesh,
            in_specs=(P('dp', None, None), P('dp', None, None), P('dp', None), P('tp', None), P(None)),
            out_specs=(P(), P('dp', None, None), P('tp', None), P(None)),
            check_vma=False)
        return sharded(hidden, residual, targets, embedding, norm_w)

    return program
```

```python
import functools

import jax
import jax.numpy as jnp
from jax import lax
from jax.experimental import pallas as pl
from jax.experimental.pallas import tpu as pltpu
from jax.sharding import PartitionSpec as P


NORM_EPS = 1e-5
CH = 256
STEP = 7
GROUPS = (1, 2, 2, 2)
PIECES = (6, 6, 6, 5, 5, 5, 5, 5, 4, 2)
ADD_AT, FINISH_AT = 1, 5
TAIL = 64
F32, BF16 = jnp.float32, jnp.bfloat16
NN = (((1,), (0,)), ((), ()))
NT = (((1,), (1,)), ((), ()))
TN = (((0,), (0,)), ((), ()))
VM = pl.BlockSpec(memory_space=pltpu.VMEM)
HB = pl.BlockSpec(memory_space=pl.ANY)


def dot(a, b, dims):
    return lax.dot_general(a, b, dims, preferred_element_type=F32)


LOG2E = 1.4426950408889634


def weights(logit, shift, hit, inv_n):
    return (jnp.exp2(logit * LOG2E + shift) - jnp.where(hit, inv_n, 0.0)).astype(BF16)


def rows_of(n, width, base):
    return lax.broadcasted_iota(jnp.int32, (n, width), 0) + base


def norm_kernel(hid_ref, res_ref, norm_ref, scaled_ref, act_ref, inv_ref):
    resid = res_ref[...] + hid_ref[...].astype(F32)
    inv = lax.rsqrt(jnp.mean(resid * resid, axis=-1, keepdims=True) + NORM_EPS)
    scaled = resid * inv
    scaled_ref[...] = scaled
    act_ref[...] = (scaled * norm_ref[...]).astype(BF16)
    inv_ref[...] = jnp.broadcast_to(inv, inv_ref.shape)


def stats_kernel(tail_rows, core_ref, emb_ref, tail_ref, ha_ref, sib_ref, norm_ref, tgt_ref, log_ref, logt_ref, stat_ref, hb_ref, top, total, hits):
    step, core = pl.program_id(0), core_ref[0]
    half = ha_ref.shape[0]

    @pl.when(step == 0)
    def _():
        top[...] = jnp.full_like(top, -jnp.inf)
        total[...] = jnp.zeros_like(total)
        hits[...] = jnp.zeros_like(hits)
        hb_ref[...] = (sib_ref[...] * norm_ref[...]).astype(BF16)

    def fold(cols, logit, hit):
        split = logit.reshape(-1, 8, half)
        new = jnp.maximum(top[:, cols], jnp.max(split, axis=0))
        total[:, cols] = total[:, cols] * jnp.exp(top[:, cols] - new) + jnp.sum(jnp.exp(split - new[None]), axis=0)
        top[:, cols] = new
        hits[:, cols] += jnp.sum(jnp.where(hit, logit, 0.0).reshape(-1, 8, half), axis=0)

    for k in range(STEP):
        rows = pl.ds(k * CH, CH)
        for side, h_ref in ((0, ha_ref), (1, hb_ref)):
            cols = pl.ds(side * half, half)
            logit = dot(emb_ref[rows, :], h_ref[...], NT)
            log_ref[rows, cols] = logit
            want = tgt_ref[0:1, cols] - (core_ref[1] + (step * STEP + k) * CH)
            fold(cols, logit, rows_of(CH, half, 0) == want)

    @pl.when(step == pl.num_programs(0) - 1)
    def _():
        for side, h_ref in ((0, ha_ref), (1, hb_ref)):
            cols = pl.ds(side * half, half)
            ids = rows_of(TAIL, half, 0)
            live = jnp.logical_and(ids < tail_rows, core == 0)
            logit = jnp.where(live, dot(tail_ref[...], h_ref[...], NT), -jnp.inf)
            logt_ref[:, cols] = logit
            fold(cols, logit, jnp.logical_and(ids + core_ref[2] == tgt_ref[0:1, cols], live))
        peak = jnp.max(top[...], axis=0, keepdims=True)
        stat_ref[...] = jnp.zeros_like(stat_ref)
        stat_ref[0:1, :] = peak
        stat_ref[1:2, :] = jnp.sum(total[...] * jnp.exp(top[...] - peak), axis=0, keepdims=True)
        stat_ref[2:3, :] = jnp.sum(hits[...], axis=0, keepdims=True)


def dh_kernel(tail_rows, inv_n, core_ref, emb_ref, log_ref, tail_ref, logt_ref, row_ref, tgt_ref, da_ref, db_ref, loss_ref, g_ref, gt_ref):
    step, core = pl.program_id(0), core_ref[0]
    half = da_ref.shape[0]

    @pl.when(step == 0)
    def _():
        loss_ref[...] = jnp.full(loss_ref.shape, jnp.sum(row_ref[1:2, pl.ds(0, half)]) + jnp.sum(row_ref[1:2, pl.ds(half, half)]))
        da_ref[...] = jnp.zeros_like(da_ref)
        db_ref[...] = jnp.zeros_like(db_ref)

    k = 0
    for group in GROUPS:
        for side, d_ref in ((0, da_ref), (1, db_ref)):
            cols = pl.ds(side * half, half)
            for i in range(k, k + group):
                rows = pl.ds(i * CH, CH)
                want = tgt_ref[0:1, cols] - (core_ref[1] + (step * STEP + i) * CH)
                g_ref[rows, cols] = weights(log_ref[rows, cols], row_ref[0:1, cols], rows_of(CH, half, 0) == want, inv_n)
            rows = pl.ds(k * CH, group * CH)
            d_ref[...] += dot(g_ref[rows, cols], emb_ref[rows, :], TN)
        k += group

    @pl.when(step == pl.num_programs(0) - 1)
    def _():
        for side, d_ref in ((0, da_ref), (1, db_ref)):
            cols = pl.ds(side * half, half)
            ids = rows_of(TAIL, half, 0)
            live = jnp.logical_and(ids < tail_rows, core == 0)
            hit = jnp.logical_and(ids + core_ref[2] == tgt_ref[0:1, cols], live)
            gt_ref[:, cols] = weights(logt_ref[:, cols], row_ref[0:1, cols], hit, inv_n)
            d_ref[...] += dot(gt_ref[:, cols], tail_ref[...], TN)


JOBS = {None: (0, 0), 'act': (3, 2), 'add': (2, 1)}


def finish_kernel(norm_ref, inv_ref, scaled_ref, near_ref, far_ref, grad_ref, sum_ref, total_ref):
    @pl.when(pl.program_id(0) == 0)
    def _():
        total_ref[...] = jnp.zeros_like(total_ref)

    grad_h, scaled = near_ref[...] + far_ref[...], scaled_ref[...]
    total_ref[...] += jnp.sum((grad_h * scaled).reshape(-1, 8, scaled.shape[1]), axis=0)
    grad_scaled = grad_h * norm_ref[...]
    mean = jnp.mean(grad_scaled * scaled, axis=-1, keepdims=True)
    grad_ref[...] = inv_ref[:, 0:1] * (grad_scaled - scaled * mean)
    sum_ref[...] = jnp.sum(total_ref[...], axis=0, keepdims=True)


def rows_at(core, first, count):
    return pl.ds(pl.multiple_of((core * sum(PIECES) + first) * CH, CH), count * CH)


def grad_kernel(job, first, count, prev, late, inv_n, core_ref, emb_ref, log_ref, ha_ref, hb_ref, hc_ref, hd_ref, row_ref, rowx_ref, mark_ref, *refs):
    per_core = sum(PIECES)
    refs = list(refs)
    if prev:
        refs = refs[3:]
    own_ref = refs.pop(0) if prev else None
    got_ref = refs.pop(0) if late else None
    jobs_in = [refs.pop(0) for _ in range(JOBS[job][0])]
    jobs_out = [refs.pop(5) for _ in range(JOBS[job][1])]
    out_ref, emb_buf, log_buf, piece_ref, token_ref, ga_ref, gx_ref, lx_ref, emb_sem, log_sem, own_sem, got_sem = refs
    core = core_ref[0]
    half = ha_ref.shape[0]
    token_ref[...] = mark_ref[...]

    def fetch(k):
        slot = lax.rem(k, 2)
        mine = pl.ds(pl.multiple_of(k * CH, CH), CH)
        return (pltpu.make_async_copy(emb_ref.at[rows_at(core, k, 1)], emb_buf.at[slot], emb_sem),
                pltpu.make_async_copy(log_ref.at[mine], log_buf.at[slot], log_sem))

    writes = []
    if prev:
        writes.append(pltpu.make_async_copy(own_ref, out_ref.at[rows_at(core, *prev)], own_sem))
    if late:
        writes.append(pltpu.make_async_copy(got_ref, out_ref.at[rows_at(1 - core, *late)], got_sem))
    if not prev:
        for copy in fetch(jnp.int32(first)):
            copy.start()
        for copy in fetch(jnp.int32(first)):
            copy.wait()
    for copy in writes:
        copy.start()
    if job == 'act':
        norm_ref, *src = jobs_in
        for src_ref, dst_ref in zip(src, jobs_out):
            dst_ref[...] = (src_ref[...] * norm_ref[...]).astype(BF16)
        hc_ref, hd_ref = jobs_out
    if job == 'add':
        jobs_out[0][...] = jobs_in[0][...] + jobs_in[1][...]

    def step(i, carry):
        k = first + i
        slot = lax.rem(k, 2)
        rows = pl.ds(pl.multiple_of(i * CH, CH), CH)
        more = k + 1 < per_core

        @pl.when(more)
        def _():
            for copy in fetch(k + 1):
                copy.start()

        base = core_ref[1] + k * CH
        for side in (0, 1):
            cols = pl.ds(side * half, half)
            want = row_ref[2:3, cols].astype(jnp.int32) - base
            ga_ref[:, cols] = weights(log_buf[slot, :, cols], row_ref[0:1, cols], rows_of(CH, half, 0) == want, inv_n)
        for side, h_ref in ((0, hc_ref), (1, hd_ref)):
            cols = pl.ds(side * half, half)
            lx_ref[:, cols] = dot(emb_buf[slot], h_ref[...], NT)
        piece_ref[rows, :] = dot(ga_ref[:, pl.ds(0, half)], ha_ref[...], NN) + dot(ga_ref[:, pl.ds(half, half)], hb_ref[...], NN)
        for side in (0, 1):
            cols = pl.ds(side * half, half)
            want = rowx_ref[2:3, cols].astype(jnp.int32) - base
            gx_ref[:, cols] = weights(lx_ref[:, cols], rowx_ref[0:1, cols], rows_of(CH, half, 0) == want, inv_n)
        piece_ref[rows, :] += dot(gx_ref[:, pl.ds(0, half)], hc_ref[...], NN) + dot(gx_ref[:, pl.ds(half, half)], hd_ref[...], NN)

        @pl.when(more)
        def _():
            for copy in fetch(k + 1):
                copy.wait()

        return carry

    lax.fori_loop(0, count, step, 0)
    for copy in writes:
        copy.wait()


def tail_kernel(inv_n, core_ref, tail_ref, ha_ref, hb_ref, hc_ref, hd_ref, row_ref, rowx_ref, _, out_ref, g_ref):
    half = ha_ref.shape[0]
    grad = jnp.zeros(out_ref.shape, F32)
    ids = rows_of(TAIL, half, 0)
    for h_ref, r_ref, side in ((ha_ref, row_ref, 0), (hb_ref, row_ref, 1), (hc_ref, rowx_ref, 0), (hd_ref, rowx_ref, 1)):
        cols = pl.ds(side * half, half)
        logit = dot(tail_ref[...], h_ref[...], NT)
        g_ref[...] = weights(logit, r_ref[0:1, cols], ids + core_ref[2] == r_ref[2:3, cols].astype(jnp.int32), inv_n)
        grad += dot(g_ref[...], h_ref[...], NN)
    out_ref[...] = grad


def last_kernel(places, core_ref, _, *refs):
    srcs, out_ref, sems = refs[:len(places)], refs[len(places)], refs[len(places) + 1:]
    copies = []
    for src, sem, (other, place) in zip(srcs, sems, places):
        side = 1 - core_ref[0] if other else core_ref[0]
        copies.append(pltpu.make_async_copy(src, out_ref.at[rows_at(side, *place)], sem))
    for copy in copies:
        copy.start()
    for copy in copies:
        copy.wait()


def cost(flops, moved):
    return pl.CostEstimate(flops=int(flops), bytes_accessed=int(moved), transcendentals=0)


def params(mib):
    return pltpu.CompilerParams(vmem_limit_bytes=mib << 20)


def swapped(value, axis, perm):
    return lax.ppermute(value, axis, perm)


def solution(mesh):
    n_tp, n_dp = mesh.shape['tp'], mesh.shape['dp']

    def program(hidden, residual, targets, embedding, norm_w):
        inv_n = 1.0 / (hidden.shape[0] * hidden.shape[1])

        def local_part(hid_loc, res_loc, tgt_loc, emb_loc, norm_vec):
            n_batch, n_seq, d = hid_loc.shape
            half = n_batch * n_seq
            vocab_loc = emb_loc.shape[0]
            per_core = sum(PIECES)
            tail_rows = vocab_loc - 2 * per_core * CH
            my_tp, my_dp = lax.axis_index('tp'), lax.axis_index('dp')
            core = lax.rem(my_dp, 2)
            start = my_tp * vocab_loc
            core_arg = jnp.stack([core, start + core * (per_core * CH), start + 2 * per_core * CH])
            swap = [(i, i ^ 1) for i in range(n_dp)]
            cross = [(i, i ^ 2) for i in range(n_dp)]
            cross_swap = [(i, i ^ 3) for i in range(n_dp)]
            flip = [(i, i ^ 1) for i in range(n_tp)]
            flip_swap = [(t * n_dp + i, (t ^ 1) * n_dp + (i ^ 1)) for t in range(n_tp) for i in range(n_dp)]

            norm_row = norm_vec.reshape(1, d)
            tgt_own = tgt_loc.reshape(1, half)
            rows = half // 4
            scaled, ha, inv_rms = pl.pallas_call(
                norm_kernel,
                grid=(4,),
                in_specs=[pl.BlockSpec((rows, d), lambda i: (i, 0)), pl.BlockSpec((rows, d), lambda i: (i, 0)), VM],
                out_specs=[pl.BlockSpec((rows, d), lambda i: (i, 0)), pl.BlockSpec((rows, d), lambda i: (i, 0)), pl.BlockSpec((rows, 128), lambda i: (i, 0))],
                out_shape=[jax.ShapeDtypeStruct((half, d), F32), jax.ShapeDtypeStruct((half, d), BF16), jax.ShapeDtypeStruct((half, 128), F32)],
                compiler_params=params(14),
                cost_estimate=cost(1e7, half * d * 12),
            )(hid_loc.reshape(half, d), res_loc.reshape(half, d), norm_row)
            scaled_sib = lax.ppermute(scaled, 'dp', swap)
            tgt_sib = lax.ppermute(tgt_own, 'dp', swap)
            scaled_far = swapped(scaled, 'dp', cross)
            tgt_near = jnp.concatenate([tgt_own, tgt_sib], axis=1)
            emb_tail = jnp.pad(emb_loc[2 * per_core * CH:], ((0, TAIL - tail_rows), (0, 0)))

            steps, blk = per_core // STEP, STEP * CH
            flops_unit = 2.0 * CH * d * half
            logits, logits_tail, stat, hb = pl.pallas_call(
                functools.partial(stats_kernel, tail_rows),
                grid_spec=pltpu.PrefetchScalarGridSpec(
                    num_scalar_prefetch=1, grid=(steps,),
                    in_specs=[pl.BlockSpec((blk, d), lambda i, c: (c[0] * steps + i, 0)), VM, VM, VM, VM, VM],
                    out_specs=[pl.BlockSpec((blk, 2 * half), lambda i, c: (i, 0)), VM, VM, VM],
                    scratch_shapes=[pltpu.VMEM((8, 2 * half), F32)] * 3),
                out_shape=[jax.ShapeDtypeStruct((per_core * CH, 2 * half), F32),
                           jax.ShapeDtypeStruct((TAIL, 2 * half), F32), jax.ShapeDtypeStruct((8, 2 * half), F32), jax.ShapeDtypeStruct((half, d), BF16)],
                compiler_params=params(30),
                cost_estimate=cost(flops_unit * per_core * 2, per_core * CH * (2 * d + 8 * half)),
            )(core_arg, emb_loc, emb_tail, ha, scaled_sib, norm_row, tgt_near)

            def turned(x):
                return jnp.concatenate([x[:, half:], x[:, :half]], axis=1)

            near = stat[0:3]
            sib = turned(lax.ppermute(near, 'dp', swap))
            over = lax.ppermute(near, 'tp', flip)
            over_sib = turned(lax.ppermute(near, ('tp', 'dp'), flip_swap))
            top = jnp.maximum(jnp.maximum(near[0], sib[0]), jnp.maximum(over[0], over_sib[0]))
            parts = [p[1] * jnp.exp(p[0] - top) for p in (near, sib, over, over_sib)]
            sum_exp = (parts[0] + parts[1]) + (parts[2] + parts[3])
            tgt_logit = (near[2] + sib[2]) + (over[2] + over_sib[2])
            token_loss = top + jnp.log(sum_exp) - tgt_logit
            row_near = jnp.pad(jnp.stack([jnp.log2(inv_n / sum_exp) - top * LOG2E, token_loss, tgt_near[0].astype(F32)]), ((0, 5), (0, 0)))
            row_near, scaled_far = lax.optimization_barrier((row_near, scaled_far))
            scaled_far_sib = swapped(scaled_far, 'dp', swap)
            row_far = swapped(row_near, 'dp', cross)

            dh_own, dh_sib, loss_chip = pl.pallas_call(
                functools.partial(dh_kernel, tail_rows, inv_n),
                grid_spec=pltpu.PrefetchScalarGridSpec(
                    num_scalar_prefetch=1, grid=(steps,),
                    in_specs=[pl.BlockSpec((blk, d), lambda i, c: (c[0] * steps + i, 0)),
                              pl.BlockSpec((blk, 2 * half), lambda i, c: (i, 0)), VM, VM, VM, VM],
                    out_specs=[VM, VM, VM],
                    scratch_shapes=[pltpu.VMEM((blk, 2 * half), BF16), pltpu.VMEM((TAIL, 2 * half), BF16)]),
                out_shape=[jax.ShapeDtypeStruct((half, d), F32)] * 2 + [jax.ShapeDtypeStruct((8, 128), F32)],
                compiler_params=params(31),
                cost_estimate=cost(flops_unit * per_core * 2, per_core * CH * (2 * d + 8 * half)),
            )(core_arg, emb_loc, logits, emb_tail, logits_tail, row_near, tgt_near)

            tie = lax.optimization_barrier
            row_near, row_far, scaled_far, scaled_far_sib, dh_own, dh_sib = tie(
                (row_near, row_far, scaled_far, scaled_far_sib, dh_own, dh_sib))
            dh_got = swapped(dh_sib, 'dp', swap)
            loss_far = swapped(loss_chip, 'dp', cross)

            def piece_call(first, count, mark, out, bufs, prev, own, late, got, far, job, job_args, job_outs):
                extra = ([] if out is None else [out, *bufs, own]) + ([] if got is None else [got]) + job_args
                specs = ([] if out is None else [HB, VM, VM, VM]) + ([] if got is None else [VM]) + [VM] * len(job_args)
                return pl.pallas_call(
                    functools.partial(grad_kernel, job, first, count, prev, late, inv_n),
                    in_specs=[pl.BlockSpec(memory_space=pltpu.SMEM), HB, HB] + [VM] * 7 + specs,
                    out_specs=[HB] + [VM] * (4 + len(job_outs)),
                    scratch_shapes=[pltpu.VMEM((CH, 2 * half), BF16), pltpu.VMEM((CH, 2 * half), BF16), pltpu.VMEM((CH, 2 * half), F32)]
                    + [pltpu.SemaphoreType.DMA] * 4,
                    out_shape=[jax.ShapeDtypeStruct((vocab_loc, d), F32), jax.ShapeDtypeStruct((2, CH, d), BF16),
                               jax.ShapeDtypeStruct((2, CH, 2 * half), F32), pltpu.VMEM((count * CH, d), F32),
                               jax.ShapeDtypeStruct((8, 128), F32)] + job_outs,
                    input_output_aliases={} if out is None else {10: 0, 11: 1, 12: 2},
                    compiler_params=params(8 if job is None else 10),
                    cost_estimate=cost(flops_unit * count * 6, count * CH * (2 * d + 8 * half + 8 * d)),
                )(core_arg, emb_loc, logits, ha, hb, *far, row_near, row_far, mark, *extra)

            out, bufs, first, own, prev, arrived = None, (), 0, None, None, []
            mark = jnp.zeros((8, 128), F32)
            far = (ha, hb)
            for k, count in enumerate(PIECES):
                late, got = arrived[k - 2] if k >= 2 else (None, None)
                job, job_args, job_outs = None, [], []
                if k == 0:
                    job, job_args = 'act', [norm_row, scaled_far, scaled_far_sib]
                    job_outs = [jax.ShapeDtypeStruct((half, d), BF16)] * 2
                if k == ADD_AT:
                    dh_got, mark = tie((dh_got, mark))
                    job, job_args, job_outs = 'add', [dh_own, dh_got], [jax.ShapeDtypeStruct((half, d), F32)]
                out, emb_buf, log_buf, piece, mark, *made = piece_call(
                    first, count, mark, out, bufs, prev, own, late, got, far, job, job_args, job_outs)
                bufs = (emb_buf, log_buf)
                own, prev = piece, (first, count)
                arrived.append((prev, lax.ppermute(piece, 'dp', swap)))
                first += count
                if k == 0:
                    far = made
                if k == ADD_AT:
                    loss_far, mark = tie((loss_far, mark))
                    dh_chip, mark = tie((made[0], mark))
                    dh_far = swapped(dh_chip, 'tp', flip)
                if k == FINISH_AT:
                    dh_far, mark = tie((dh_far, mark))
                    blk_rows = pl.BlockSpec((half // 4, d), lambda i: (i, 0))
                    grad_r, grad_w = pl.pallas_call(
                        finish_kernel,
                        grid=(4,),
                        in_specs=[VM, pl.BlockSpec((half // 4, 128), lambda i: (i, 0)), blk_rows, blk_rows, blk_rows],
                        out_specs=[blk_rows, VM],
                        scratch_shapes=[pltpu.VMEM((8, d), F32)],
                        out_shape=[jax.ShapeDtypeStruct((half, d), F32), jax.ShapeDtypeStruct((1, d), F32)],
                        compiler_params=params(8),
                        cost_estimate=cost(1e7, half * d * 16),
                    )(norm_row, inv_rms, scaled, dh_chip, dh_far)
                    grad_w, mark = tie((grad_w, mark))
                    gw = [swapped(grad_w, 'dp', swap), swapped(grad_w, 'dp', cross), swapped(grad_w, 'dp', cross_swap)]
            loss_mean = ((loss_chip + loss_far) * inv_n)[0, 0]
            grad_w = ((grad_w + gw[0]) + (gw[1] + gw[2])).reshape(d)
            hc, hd = far

            out = pl.pallas_call(
                functools.partial(tail_kernel, inv_n),
                grid_spec=pltpu.PrefetchScalarGridSpec(
                    num_scalar_prefetch=1, grid=(1,), in_specs=[VM] * 7 + [HB],
                    out_specs=pl.BlockSpec((TAIL, d), lambda i, c: (2 * per_core * CH // TAIL, 0)),
                    scratch_shapes=[pltpu.VMEM((TAIL, half), BF16)]),
                out_shape=jax.ShapeDtypeStruct((vocab_loc, d), F32),
                input_output_aliases={8: 0},
                compiler_params=params(14),
                cost_estimate=cost(2.0 * TAIL * d * half * 8, 4 * TAIL * d),
            )(core_arg, emb_tail, ha, hb, hc, hd, row_near, row_far, out)
            for parts in ([(False, prev, own), (True, *arrived[-2])], [(True, *arrived[-1])]):
                out = pl.pallas_call(
                    functools.partial(last_kernel, [p[:2] for p in parts]),
                    in_specs=[pl.BlockSpec(memory_space=pltpu.SMEM), HB] + [VM] * len(parts), out_specs=HB,
                    scratch_shapes=[pltpu.SemaphoreType.DMA] * len(parts),
                    out_shape=jax.ShapeDtypeStruct((vocab_loc, d), F32),
                    input_output_aliases={1: 0},
                    compiler_params=params(8),
                    cost_estimate=cost(1e6, sum(4 * p[1][1] * CH * d for p in parts)),
                )(core_arg, out, *[p[2] for p in parts])
            return loss_mean, grad_r.reshape(n_batch, n_seq, d), out, grad_w

        sharded = jax.shard_map(
            local_part, mesh=mesh,
            in_specs=(P('dp', None, None), P('dp', None, None), P('dp', None), P('tp', None), P(None)),
            out_specs=(P(), P('dp', None, None), P('tp', None), P(None)),
            check_vma=False)
        return sharded(hidden, residual, targets, embedding, norm_w)

    return program
```

```python
import functools

import jax
import jax.numpy as jnp
from jax import lax
from jax.experimental import pallas as pl
from jax.experimental.pallas import tpu as pltpu
from jax.sharding import PartitionSpec as P


NORM_EPS = 1e-5
CH = 256
STEP = 7
GROUPS = (1, 2, 2, 2)
PIECES = (6, 6, 6, 5, 5, 5, 5, 5, 4, 2)
ADD_AT, FINISH_AT = 1, 5
TAIL = 64
F32, BF16 = jnp.float32, jnp.bfloat16
NN = (((1,), (0,)), ((), ()))
NT = (((1,), (1,)), ((), ()))
TN = (((0,), (0,)), ((), ()))
VM = pl.BlockSpec(memory_space=pltpu.VMEM)
HB = pl.BlockSpec(memory_space=pl.ANY)


def dot(a, b, dims):
    return lax.dot_general(a, b, dims, preferred_element_type=F32)


LOG2E = 1.4426950408889634


def weights(logit, shift, hit, inv_n):
    return (jnp.exp2(logit * LOG2E + shift) - jnp.where(hit, inv_n, 0.0)).astype(BF16)


def seat(vocab_loc):
    core, start, span = lax.rem(lax.axis_index('dp'), 2), lax.axis_index('tp') * vocab_loc, sum(PIECES) * CH
    return core, start + core * span, start + 2 * span


def rows_of(n, width, base):
    return lax.broadcasted_iota(jnp.int32, (n, width), 0) + base


def norm_kernel(hid_ref, res_ref, norm_ref, scaled_ref, act_ref, inv_ref):
    resid = res_ref[...] + hid_ref[...].astype(F32)
    inv = lax.rsqrt(jnp.mean(resid * resid, axis=-1, keepdims=True) + NORM_EPS)
    scaled = resid * inv
    scaled_ref[...] = scaled
    act_ref[...] = (scaled * norm_ref[...]).astype(BF16)
    inv_ref[...] = jnp.broadcast_to(inv, inv_ref.shape)


def stats_kernel(tail_rows, core_ref, emb_ref, tail_ref, ha_ref, sib_ref, norm_ref, tgt_ref, log_ref, logt_ref, stat_ref, hb_ref, top, total, hits):
    step = pl.program_id(0)
    core, base, tail_base = seat(2 * sum(PIECES) * CH + tail_rows)
    half = ha_ref.shape[0]

    @pl.when(step == 0)
    def _():
        top[...] = jnp.full_like(top, -jnp.inf)
        total[...] = jnp.zeros_like(total)
        hits[...] = jnp.zeros_like(hits)
        hb_ref[...] = (sib_ref[...] * norm_ref[...]).astype(BF16)

    def fold(cols, logit, hit):
        split = logit.reshape(-1, 8, half)
        new = jnp.maximum(top[:, cols], jnp.max(split, axis=0))
        total[:, cols] = total[:, cols] * jnp.exp(top[:, cols] - new) + jnp.sum(jnp.exp(split - new[None]), axis=0)
        top[:, cols] = new
        hits[:, cols] += jnp.sum(jnp.where(hit, logit, 0.0).reshape(-1, 8, half), axis=0)

    for k in range(STEP):
        rows = pl.ds(k * CH, CH)
        for side, h_ref in ((0, ha_ref), (1, hb_ref)):
            cols = pl.ds(side * half, half)
            logit = dot(emb_ref[rows, :], h_ref[...], NT)
            log_ref[rows, cols] = logit
            want = tgt_ref[0:1, cols] - (base + (step * STEP + k) * CH)
            fold(cols, logit, rows_of(CH, half, 0) == want)

    @pl.when(step == pl.num_programs(0) - 1)
    def _():
        for side, h_ref in ((0, ha_ref), (1, hb_ref)):
            cols = pl.ds(side * half, half)
            ids = rows_of(TAIL, half, 0)
            live = jnp.logical_and(ids < tail_rows, core == 0)
            logit = jnp.where(live, dot(tail_ref[...], h_ref[...], NT), -jnp.inf)
            logt_ref[:, cols] = logit
            fold(cols, logit, jnp.logical_and(ids + tail_base == tgt_ref[0:1, cols], live))
        peak = jnp.max(top[...], axis=0, keepdims=True)
        stat_ref[...] = jnp.zeros_like(stat_ref)
        stat_ref[0:1, :] = peak
        stat_ref[1:2, :] = jnp.sum(total[...] * jnp.exp(top[...] - peak), axis=0, keepdims=True)
        stat_ref[2:3, :] = jnp.sum(hits[...], axis=0, keepdims=True)


def dh_kernel(tail_rows, inv_n, core_ref, emb_ref, log_ref, tail_ref, logt_ref, row_ref, tgt_ref, da_ref, db_ref, loss_ref, g_ref, gt_ref):
    step = pl.program_id(0)
    core, base, tail_base = seat(2 * sum(PIECES) * CH + tail_rows)
    half = da_ref.shape[0]

    @pl.when(step == 0)
    def _():
        loss_ref[...] = jnp.full(loss_ref.shape, jnp.sum(row_ref[1:2, pl.ds(0, half)]) + jnp.sum(row_ref[1:2, pl.ds(half, half)]))
        da_ref[...] = jnp.zeros_like(da_ref)
        db_ref[...] = jnp.zeros_like(db_ref)

    k = 0
    for group in GROUPS:
        for side, d_ref in ((0, da_ref), (1, db_ref)):
            cols = pl.ds(side * half, half)
            for i in range(k, k + group):
                rows = pl.ds(i * CH, CH)
                want = tgt_ref[0:1, cols] - (base + (step * STEP + i) * CH)
                g_ref[rows, cols] = weights(log_ref[rows, cols], row_ref[0:1, cols], rows_of(CH, half, 0) == want, inv_n)
            rows = pl.ds(k * CH, group * CH)
            d_ref[...] += dot(g_ref[rows, cols], emb_ref[rows, :], TN)
        k += group

    @pl.when(step == pl.num_programs(0) - 1)
    def _():
        for side, d_ref in ((0, da_ref), (1, db_ref)):
            cols = pl.ds(side * half, half)
            ids = rows_of(TAIL, half, 0)
            live = jnp.logical_and(ids < tail_rows, core == 0)
            hit = jnp.logical_and(ids + tail_base == tgt_ref[0:1, cols], live)
            gt_ref[:, cols] = weights(logt_ref[:, cols], row_ref[0:1, cols], hit, inv_n)
            d_ref[...] += dot(gt_ref[:, cols], tail_ref[...], TN)


JOBS = {None: (0, 0), 'act': (3, 2), 'add': (2, 1)}


def finish_kernel(norm_ref, inv_ref, loss_ref, scaled_ref, near_ref, far_ref, grad_ref, sum_ref, total_ref):
    @pl.when(pl.program_id(0) == 0)
    def _():
        total_ref[...] = jnp.zeros_like(total_ref)

    grad_h, scaled = near_ref[...] + far_ref[...], scaled_ref[...]
    total_ref[...] += jnp.sum((grad_h * scaled).reshape(-1, 8, scaled.shape[1]), axis=0)
    grad_scaled = grad_h * norm_ref[...]
    mean = jnp.mean(grad_scaled * scaled, axis=-1, keepdims=True)
    grad_ref[...] = inv_ref[:, 0:1] * (grad_scaled - scaled * mean)
    sum_ref[0:1, :] = jnp.sum(total_ref[...], axis=0, keepdims=True)
    sum_ref[1:2, :] = jnp.zeros((1, sum_ref.shape[1]), F32)
    sum_ref[1:2, 0:128] = loss_ref[0:1, :]


def rows_at(core, first, count):
    return pl.ds(pl.multiple_of((core * sum(PIECES) + first) * CH, CH), count * CH)


def grad_kernel(job, first, count, prev, late, inv_n, emb_ref, log_ref, ha_ref, hb_ref, hc_ref, hd_ref, row_ref, rowx_ref, mark_ref, *refs):
    per_core = sum(PIECES)
    refs = list(refs)
    if prev:
        refs = refs[3:]
    own_ref = refs.pop(0) if prev else None
    got_ref = refs.pop(0) if late else None
    jobs_in = [refs.pop(0) for _ in range(JOBS[job][0])]
    jobs_out = [refs.pop(5) for _ in range(JOBS[job][1])]
    out_ref, emb_buf, log_buf, piece_ref, token_ref, ga_ref, gx_ref, lx_ref, emb_sem, log_sem, own_sem, got_sem = refs
    core, start, _ = seat(out_ref.shape[0])
    half = ha_ref.shape[0]
    token_ref[...] = mark_ref[...]

    def fetch(k):
        slot = lax.rem(k, 2)
        mine = pl.ds(pl.multiple_of(k * CH, CH), CH)
        return (pltpu.make_async_copy(emb_ref.at[rows_at(core, k, 1)], emb_buf.at[slot], emb_sem),
                pltpu.make_async_copy(log_ref.at[mine], log_buf.at[slot], log_sem))

    writes = []
    if prev:
        writes.append(pltpu.make_async_copy(own_ref, out_ref.at[rows_at(core, *prev)], own_sem))
    if late:
        writes.append(pltpu.make_async_copy(got_ref, out_ref.at[rows_at(1 - core, *late)], got_sem))
    if not prev:
        for copy in fetch(jnp.int32(first)):
            copy.start()
        for copy in fetch(jnp.int32(first)):
            copy.wait()
    for copy in writes:
        copy.start()
    if job == 'act':
        norm_ref, *src = jobs_in
        for src_ref, dst_ref in zip(src, jobs_out):
            dst_ref[...] = (src_ref[...] * norm_ref[...]).astype(BF16)
        hc_ref, hd_ref = jobs_out
    if job == 'add':
        jobs_out[0][...] = jobs_in[0][...] + jobs_in[1][...]

    def step(i, carry):
        k = first + i
        slot = lax.rem(k, 2)
        rows = pl.ds(pl.multiple_of(i * CH, CH), CH)
        more = k + 1 < per_core

        @pl.when(more)
        def _():
            for copy in fetch(k + 1):
                copy.start()

        base = start + k * CH
        for side in (0, 1):
            cols = pl.ds(side * half, half)
            want = row_ref[2:3, cols].astype(jnp.int32) - base
            ga_ref[:, cols] = weights(log_buf[slot, :, cols], row_ref[0:1, cols], rows_of(CH, half, 0) == want, inv_n)
        for side, h_ref in ((0, hc_ref), (1, hd_ref)):
            cols = pl.ds(side * half, half)
            lx_ref[:, cols] = dot(emb_buf[slot], h_ref[...], NT)
        piece_ref[rows, :] = dot(ga_ref[:, pl.ds(0, half)], ha_ref[...], NN) + dot(ga_ref[:, pl.ds(half, half)], hb_ref[...], NN)
        for side in (0, 1):
            cols = pl.ds(side * half, half)
            want = rowx_ref[2:3, cols].astype(jnp.int32) - base
            gx_ref[:, cols] = weights(lx_ref[:, cols], rowx_ref[0:1, cols], rows_of(CH, half, 0) == want, inv_n)
        piece_ref[rows, :] += dot(gx_ref[:, pl.ds(0, half)], hc_ref[...], NN) + dot(gx_ref[:, pl.ds(half, half)], hd_ref[...], NN)

        @pl.when(more)
        def _():
            for copy in fetch(k + 1):
                copy.wait()

        return carry

    lax.fori_loop(0, count, step, 0)
    for copy in writes:
        copy.wait()


def tail_kernel(inv_n, vocab_loc, tail_ref, ha_ref, hb_ref, hc_ref, hd_ref, row_ref, rowx_ref, *refs):
    sums, (_, out_ref, sum_ref, loss_ref, g_ref) = refs[:4], refs[4:]
    half = ha_ref.shape[0]
    _, _, tail_base = seat(vocab_loc)
    both = (sums[0][...] + sums[1][...]) + (sums[2][...] + sums[3][...])
    sum_ref[...] = both[0:1]
    loss_ref[0, 0] = jnp.sum(both[1:2, 0:128]) * (inv_n / 256)
    grad = jnp.zeros(out_ref.shape, F32)
    ids = rows_of(TAIL, half, 0)
    for h_ref, r_ref, side in ((ha_ref, row_ref, 0), (hb_ref, row_ref, 1), (hc_ref, rowx_ref, 0), (hd_ref, rowx_ref, 1)):
        cols = pl.ds(side * half, half)
        logit = dot(tail_ref[...], h_ref[...], NT)
        g_ref[...] = weights(logit, r_ref[0:1, cols], ids + tail_base == r_ref[2:3, cols].astype(jnp.int32), inv_n)
        grad += dot(g_ref[...], h_ref[...], NN)
    out_ref[...] = grad


def last_kernel(places, _, *refs):
    srcs, out_ref, sems = refs[:len(places)], refs[len(places)], refs[len(places) + 1:]
    core, _, _ = seat(out_ref.shape[0])
    copies = []
    for src, sem, (other, place) in zip(srcs, sems, places):
        side = 1 - core if other else core
        copies.append(pltpu.make_async_copy(src, out_ref.at[rows_at(side, *place)], sem))
    for copy in copies:
        copy.start()
    for copy in copies:
        copy.wait()


def cost(flops, moved):
    return pl.CostEstimate(flops=int(flops), bytes_accessed=int(moved), transcendentals=0)


def params(mib):
    return pltpu.CompilerParams(vmem_limit_bytes=mib << 20)


def swapped(value, axis, perm):
    return lax.ppermute(value, axis, perm)


def solution(mesh):
    n_tp, n_dp = mesh.shape['tp'], mesh.shape['dp']

    def program(hidden, residual, targets, embedding, norm_w):
        inv_n = 1.0 / (hidden.shape[0] * hidden.shape[1])

        def local_part(hid_loc, res_loc, tgt_loc, emb_loc, norm_vec):
            n_batch, n_seq, d = hid_loc.shape
            half = n_batch * n_seq
            vocab_loc = emb_loc.shape[0]
            per_core = sum(PIECES)
            tail_rows = vocab_loc - 2 * per_core * CH
            my_dp = lax.axis_index('dp')
            core = lax.rem(my_dp, 2)
            core_arg = core.reshape(1)
            swap = [(i, i ^ 1) for i in range(n_dp)]
            cross = [(i, i ^ 2) for i in range(n_dp)]
            cross_swap = [(i, i ^ 3) for i in range(n_dp)]
            flip = [(i, i ^ 1) for i in range(n_tp)]
            flip_swap = [(t * n_dp + i, (t ^ 1) * n_dp + (i ^ 1)) for t in range(n_tp) for i in range(n_dp)]

            norm_row = norm_vec.reshape(1, d)
            tgt_own = tgt_loc.reshape(1, half)
            rows = half // 4
            scaled, ha, inv_rms = pl.pallas_call(
                norm_kernel,
                grid=(4,),
                in_specs=[pl.BlockSpec((rows, d), lambda i: (i, 0)), pl.BlockSpec((rows, d), lambda i: (i, 0)), VM],
                out_specs=[pl.BlockSpec((rows, d), lambda i: (i, 0)), pl.BlockSpec((rows, d), lambda i: (i, 0)), pl.BlockSpec((rows, 128), lambda i: (i, 0))],
                out_shape=[jax.ShapeDtypeStruct((half, d), F32), jax.ShapeDtypeStruct((half, d), BF16), jax.ShapeDtypeStruct((half, 128), F32)],
                compiler_params=params(14),
                cost_estimate=cost(1e7, half * d * 12),
            )(hid_loc.reshape(half, d), res_loc.reshape(half, d), norm_row)
            scaled_sib = lax.ppermute(scaled, 'dp', swap)
            tgt_sib = lax.ppermute(tgt_own, 'dp', swap)
            scaled_far = swapped(scaled, 'dp', cross)
            tgt_near = jnp.concatenate([tgt_own, tgt_sib], axis=1)
            emb_tail = jnp.pad(emb_loc[2 * per_core * CH:], ((0, TAIL - tail_rows), (0, 0)))

            steps, blk = per_core // STEP, STEP * CH
            flops_unit = 2.0 * CH * d * half
            logits, logits_tail, stat, hb = pl.pallas_call(
                functools.partial(stats_kernel, tail_rows),
                grid_spec=pltpu.PrefetchScalarGridSpec(
                    num_scalar_prefetch=1, grid=(steps,),
                    in_specs=[pl.BlockSpec((blk, d), lambda i, c: (c[0] * steps + i, 0)), VM, VM, VM, VM, VM],
                    out_specs=[pl.BlockSpec((blk, 2 * half), lambda i, c: (i, 0)), VM, VM, VM],
                    scratch_shapes=[pltpu.VMEM((8, 2 * half), F32)] * 3),
                out_shape=[jax.ShapeDtypeStruct((per_core * CH, 2 * half), F32),
                           jax.ShapeDtypeStruct((TAIL, 2 * half), F32), jax.ShapeDtypeStruct((8, 2 * half), F32), jax.ShapeDtypeStruct((half, d), BF16)],
                compiler_params=params(30),
                cost_estimate=cost(flops_unit * per_core * 2, per_core * CH * (2 * d + 8 * half)),
            )(core_arg, emb_loc, emb_tail, ha, scaled_sib, norm_row, tgt_near)

            def turned(x):
                return jnp.concatenate([x[:, half:], x[:, :half]], axis=1)

            near = stat[0:3]
            sib = turned(lax.ppermute(near, 'dp', swap))
            over = lax.ppermute(near, 'tp', flip)
            over_sib = turned(lax.ppermute(near, ('tp', 'dp'), flip_swap))
            top = jnp.maximum(jnp.maximum(near[0], sib[0]), jnp.maximum(over[0], over_sib[0]))
            parts = [p[1] * jnp.exp(p[0] - top) for p in (near, sib, over, over_sib)]
            sum_exp = (parts[0] + parts[1]) + (parts[2] + parts[3])
            tgt_logit = (near[2] + sib[2]) + (over[2] + over_sib[2])
            token_loss = top + jnp.log(sum_exp) - tgt_logit
            row_near = jnp.pad(jnp.stack([jnp.log2(inv_n / sum_exp) - top * LOG2E, token_loss, tgt_near[0].astype(F32)]), ((0, 5), (0, 0)))
            row_near, scaled_far = lax.optimization_barrier((row_near, scaled_far))
            scaled_far_sib = swapped(scaled_far, 'dp', swap)
            row_far = swapped(row_near, 'dp', cross)

            dh_own, dh_sib, loss_chip = pl.pallas_call(
                functools.partial(dh_kernel, tail_rows, inv_n),
                grid_spec=pltpu.PrefetchScalarGridSpec(
                    num_scalar_prefetch=1, grid=(steps,),
                    in_specs=[pl.BlockSpec((blk, d), lambda i, c: (c[0] * steps + i, 0)),
                              pl.BlockSpec((blk, 2 * half), lambda i, c: (i, 0)), VM, VM, VM, VM],
                    out_specs=[VM, VM, VM],
                    scratch_shapes=[pltpu.VMEM((blk, 2 * half), BF16), pltpu.VMEM((TAIL, 2 * half), BF16)]),
                out_shape=[jax.ShapeDtypeStruct((half, d), F32)] * 2 + [jax.ShapeDtypeStruct((8, 128), F32)],
                compiler_params=params(31),
                cost_estimate=cost(flops_unit * per_core * 2, per_core * CH * (2 * d + 8 * half)),
            )(core_arg, emb_loc, logits, emb_tail, logits_tail, row_near, tgt_near)

            tie = lax.optimization_barrier
            row_near, row_far, scaled_far, scaled_far_sib, dh_own, dh_sib = tie(
                (row_near, row_far, scaled_far, scaled_far_sib, dh_own, dh_sib))
            dh_got = swapped(dh_sib, 'dp', swap)

            def piece_call(first, count, mark, out, bufs, prev, own, late, got, far, job, job_args, job_outs):
                extra = ([] if out is None else [out, *bufs, own]) + ([] if got is None else [got]) + job_args
                specs = ([] if out is None else [HB, VM, VM, VM]) + ([] if got is None else [VM]) + [VM] * len(job_args)
                return pl.pallas_call(
                    functools.partial(grad_kernel, job, first, count, prev, late, inv_n),
                    in_specs=[HB, HB] + [VM] * 7 + specs,
                    out_specs=[HB] + [VM] * (4 + len(job_outs)),
                    scratch_shapes=[pltpu.VMEM((CH, 2 * half), BF16), pltpu.VMEM((CH, 2 * half), BF16), pltpu.VMEM((CH, 2 * half), F32)]
                    + [pltpu.SemaphoreType.DMA] * 4,
                    out_shape=[jax.ShapeDtypeStruct((vocab_loc, d), F32), jax.ShapeDtypeStruct((2, CH, d), BF16),
                               jax.ShapeDtypeStruct((2, CH, 2 * half), F32), pltpu.VMEM((count * CH, d), F32),
                               jax.ShapeDtypeStruct((8, 128), F32)] + job_outs,
                    input_output_aliases={} if out is None else {9: 0, 10: 1, 11: 2},
                    compiler_params=params(8 if job is None else 10),
                    cost_estimate=cost(flops_unit * count * 6, count * CH * (2 * d + 8 * half + 8 * d)),
                )(emb_loc, logits, ha, hb, *far, row_near, row_far, mark, *extra)

            out, bufs, first, own, prev, arrived = None, (), 0, None, None, []
            mark = jnp.zeros((8, 128), F32)
            far = (ha, hb)
            for k, count in enumerate(PIECES):
                late, got = arrived[k - 2] if k >= 2 else (None, None)
                job, job_args, job_outs = None, [], []
                if k == 0:
                    job, job_args = 'act', [norm_row, scaled_far, scaled_far_sib]
                    job_outs = [jax.ShapeDtypeStruct((half, d), BF16)] * 2
                if k == ADD_AT:
                    dh_got, mark = tie((dh_got, mark))
                    job, job_args, job_outs = 'add', [dh_own, dh_got], [jax.ShapeDtypeStruct((half, d), F32)]
                out, emb_buf, log_buf, piece, mark, *made = piece_call(
                    first, count, mark, out, bufs, prev, own, late, got, far, job, job_args, job_outs)
                bufs = (emb_buf, log_buf)
                own, prev = piece, (first, count)
                arrived.append((prev, lax.ppermute(piece, 'dp', swap)))
                first += count
                if k == 0:
                    far = made
                if k == ADD_AT:
                    dh_chip, mark = tie((made[0], mark))
                    dh_far = swapped(dh_chip, 'tp', flip)
                if k == FINISH_AT:
                    dh_far, mark = tie((dh_far, mark))
                    blk_rows = pl.BlockSpec((half // 4, d), lambda i: (i, 0))
                    grad_r, grad_w = pl.pallas_call(
                        finish_kernel,
                        grid=(4,),
                        in_specs=[VM, pl.BlockSpec((half // 4, 128), lambda i: (i, 0)), VM, blk_rows, blk_rows, blk_rows],
                        out_specs=[blk_rows, VM],
                        scratch_shapes=[pltpu.VMEM((8, d), F32)],
                        out_shape=[jax.ShapeDtypeStruct((half, d), F32), jax.ShapeDtypeStruct((2, d), F32)],
                        compiler_params=params(8),
                        cost_estimate=cost(1e7, half * d * 16),
                    )(norm_row, inv_rms, loss_chip, scaled, dh_chip, dh_far)
                    grad_w, mark = tie((grad_w, mark))
                    gw = [swapped(grad_w, 'dp', swap), swapped(grad_w, 'dp', cross), swapped(grad_w, 'dp', cross_swap)]
            hc, hd = far

            out, grad_w, loss_mean = pl.pallas_call(
                functools.partial(tail_kernel, inv_n, vocab_loc),
                grid=(1,), in_specs=[VM] * 11 + [HB],
                out_specs=[pl.BlockSpec((TAIL, d), lambda i: (2 * per_core * CH // TAIL, 0)), VM, pl.BlockSpec(memory_space=pltpu.SMEM)],
                scratch_shapes=[pltpu.VMEM((TAIL, half), BF16)],
                out_shape=[jax.ShapeDtypeStruct((vocab_loc, d), F32), jax.ShapeDtypeStruct((1, d), F32), jax.ShapeDtypeStruct((1, 1), F32)],
                input_output_aliases={11: 0},
                compiler_params=params(14),
                cost_estimate=cost(2.0 * TAIL * d * half * 8, 4 * TAIL * d),
            )(emb_tail, ha, hb, hc, hd, row_near, row_far, grad_w, *gw, out)
            for parts in ([(False, prev, own), (True, *arrived[-2])], [(True, *arrived[-1])]):
                out = pl.pallas_call(
                    functools.partial(last_kernel, [p[:2] for p in parts]),
                    in_specs=[HB] + [VM] * len(parts), out_specs=HB,
                    scratch_shapes=[pltpu.SemaphoreType.DMA] * len(parts),
                    out_shape=jax.ShapeDtypeStruct((vocab_loc, d), F32),
                    input_output_aliases={0: 0},
                    compiler_params=params(8),
                    cost_estimate=cost(1e6, sum(4 * p[1][1] * CH * d for p in parts)),
                )(out, *[p[2] for p in parts])
            return loss_mean.reshape(()), grad_r.reshape(n_batch, n_seq, d), out, grad_w.reshape(d)

        sharded = jax.shard_map(
            local_part, mesh=mesh,
            in_specs=(P('dp', None, None), P('dp', None, None), P('dp', None), P('tp', None), P(None)),
            out_specs=(P(), P('dp', None, None), P('tp', None), P(None)),
            check_vma=False)
        return sharded(hidden, residual, targets, embedding, norm_w)

    return program
```

```python
import functools

import jax
import jax.numpy as jnp
from jax import lax
from jax.experimental import pallas as pl
from jax.experimental.pallas import tpu as pltpu
from jax.sharding import PartitionSpec as P


NORM_EPS = 1e-5
CH = 256
STEP = 7
GROUPS = (1, 2, 2, 2)
PIECES = (5, 6, 5, 6, 5, 6, 5, 5, 4, 2)
ADD_AT, FINISH_AT = 1, 5
TAIL = 64
F32, BF16 = jnp.float32, jnp.bfloat16
NN = (((1,), (0,)), ((), ()))
NT = (((1,), (1,)), ((), ()))
TN = (((0,), (0,)), ((), ()))
VM = pl.BlockSpec(memory_space=pltpu.VMEM)
HB = pl.BlockSpec(memory_space=pl.ANY)


def dot(a, b, dims):
    return lax.dot_general(a, b, dims, preferred_element_type=F32)


LOG2E = 1.4426950408889634


def weights(logit, shift, hit, inv_n):
    return (jnp.exp2(logit * LOG2E + shift) - jnp.where(hit, inv_n, 0.0)).astype(BF16)


def seat(vocab_loc):
    core, start, span = lax.rem(lax.axis_index('dp'), 2), lax.axis_index('tp') * vocab_loc, sum(PIECES) * CH
    return core, start + core * span, start + 2 * span


def rows_of(n, width, base):
    return lax.broadcasted_iota(jnp.int32, (n, width), 0) + base


def norm_kernel(hid_ref, res_ref, norm_ref, scaled_ref, act_ref, inv_ref):
    resid = res_ref[...] + hid_ref[...].astype(F32)
    inv = lax.rsqrt(jnp.mean(resid * resid, axis=-1, keepdims=True) + NORM_EPS)
    scaled = resid * inv
    scaled_ref[...] = scaled
    act_ref[...] = (scaled * norm_ref[...]).astype(BF16)
    inv_ref[...] = jnp.broadcast_to(inv, inv_ref.shape)


def stats_kernel(tail_rows, core_ref, emb_ref, tail_ref, ha_ref, sib_ref, norm_ref, tgt_ref, log_ref, logt_ref, stat_ref, hb_ref, top, total, hits, wa_ref, wb_ref):
    step = pl.program_id(0)
    core, base, tail_base = seat(2 * sum(PIECES) * CH + tail_rows)
    half = ha_ref.shape[0]

    @pl.when(step == 0)
    def _():
        top[...] = jnp.full_like(top, -jnp.inf)
        total[...] = jnp.zeros_like(total)
        hits[...] = jnp.zeros_like(hits)
        hb_ref[...] = (sib_ref[...] * norm_ref[...]).astype(BF16)
        wa_ref[...] = ha_ref[...].T
        wb_ref[...] = hb_ref[...].T

    def fold(cols, logit, hit):
        split = logit.reshape(-1, 8, half)
        new = jnp.maximum(top[:, cols], jnp.max(split, axis=0))
        total[:, cols] = total[:, cols] * jnp.exp(top[:, cols] - new) + jnp.sum(jnp.exp(split - new[None]), axis=0)
        top[:, cols] = new
        hits[:, cols] += jnp.sum(jnp.where(hit, logit, 0.0).reshape(-1, 8, half), axis=0)

    for k in range(STEP):
        rows = pl.ds(k * CH, CH)
        for side, h_ref in ((0, wa_ref), (1, wb_ref)):
            cols = pl.ds(side * half, half)
            logit = dot(emb_ref[rows, :], h_ref[...], NN)
            log_ref[rows, cols] = logit
            want = tgt_ref[0:1, cols] - (base + (step * STEP + k) * CH)
            fold(cols, logit, rows_of(CH, half, 0) == want)

    @pl.when(step == pl.num_programs(0) - 1)
    def _():
        for side, h_ref in ((0, wa_ref), (1, wb_ref)):
            cols = pl.ds(side * half, half)
            ids = rows_of(TAIL, half, 0)
            live = jnp.logical_and(ids < tail_rows, core == 0)
            logit = jnp.where(live, dot(tail_ref[...], h_ref[...], NN), -jnp.inf)
            logt_ref[:, cols] = logit
            fold(cols, logit, jnp.logical_and(ids + tail_base == tgt_ref[0:1, cols], live))
        peak = jnp.max(top[...], axis=0, keepdims=True)
        stat_ref[...] = jnp.zeros_like(stat_ref)
        stat_ref[0:1, :] = peak
        stat_ref[1:2, :] = jnp.sum(total[...] * jnp.exp(top[...] - peak), axis=0, keepdims=True)
        stat_ref[2:3, :] = jnp.sum(hits[...], axis=0, keepdims=True)


def dh_kernel(tail_rows, inv_n, core_ref, emb_ref, log_ref, tail_ref, logt_ref, row_ref, tgt_ref, da_ref, db_ref, loss_ref, g_ref, gt_ref):
    step = pl.program_id(0)
    core, base, tail_base = seat(2 * sum(PIECES) * CH + tail_rows)
    half = da_ref.shape[0]

    @pl.when(step == 0)
    def _():
        loss_ref[...] = jnp.full(loss_ref.shape, jnp.sum(row_ref[1:2, pl.ds(0, half)]) + jnp.sum(row_ref[1:2, pl.ds(half, half)]))
        da_ref[...] = jnp.zeros_like(da_ref)
        db_ref[...] = jnp.zeros_like(db_ref)

    k = 0
    for group in GROUPS:
        for side, d_ref in ((0, da_ref), (1, db_ref)):
            cols = pl.ds(side * half, half)
            for i in range(k, k + group):
                rows = pl.ds(i * CH, CH)
                want = tgt_ref[0:1, cols] - (base + (step * STEP + i) * CH)
                g_ref[rows, cols] = weights(log_ref[rows, cols], row_ref[0:1, cols], rows_of(CH, half, 0) == want, inv_n)
            rows = pl.ds(k * CH, group * CH)
            d_ref[...] += dot(g_ref[rows, cols], emb_ref[rows, :], TN)
        k += group

    @pl.when(step == pl.num_programs(0) - 1)
    def _():
        for side, d_ref in ((0, da_ref), (1, db_ref)):
            cols = pl.ds(side * half, half)
            ids = rows_of(TAIL, half, 0)
            live = jnp.logical_and(ids < tail_rows, core == 0)
            hit = jnp.logical_and(ids + tail_base == tgt_ref[0:1, cols], live)
            gt_ref[:, cols] = weights(logt_ref[:, cols], row_ref[0:1, cols], hit, inv_n)
            d_ref[...] += dot(gt_ref[:, cols], tail_ref[...], TN)


JOBS = {None: (0, 0), 'act': (3, 4), 'add': (2, 1)}


def finish_kernel(norm_ref, inv_ref, loss_ref, scaled_ref, near_ref, far_ref, grad_ref, sum_ref, total_ref):
    @pl.when(pl.program_id(0) == 0)
    def _():
        total_ref[...] = jnp.zeros_like(total_ref)

    grad_h, scaled = near_ref[...] + far_ref[...], scaled_ref[...]
    total_ref[...] += jnp.sum((grad_h * scaled).reshape(-1, 8, scaled.shape[1]), axis=0)
    grad_scaled = grad_h * norm_ref[...]
    mean = jnp.mean(grad_scaled * scaled, axis=-1, keepdims=True)
    grad_ref[...] = inv_ref[:, 0:1] * (grad_scaled - scaled * mean)
    sum_ref[0:1, :] = jnp.sum(total_ref[...], axis=0, keepdims=True)
    sum_ref[1:2, :] = jnp.zeros((1, sum_ref.shape[1]), F32)
    sum_ref[1:2, 0:128] = loss_ref[0:1, :]


def rows_at(core, first, count):
    return pl.ds(pl.multiple_of((core * sum(PIECES) + first) * CH, CH), count * CH)


def grad_kernel(job, first, count, prev, late, inv_n, emb_ref, log_ref, ha_ref, hb_ref, hc_ref, hd_ref, xc_ref, xd_ref, row_ref, rowx_ref, mark_ref, *refs):
    per_core = sum(PIECES)
    refs = list(refs)
    if prev:
        refs = refs[3:]
    own_ref = refs.pop(0) if prev else None
    got_ref = refs.pop(0) if late else None
    jobs_in = [refs.pop(0) for _ in range(JOBS[job][0])]
    jobs_out = [refs.pop(5) for _ in range(JOBS[job][1])]
    out_ref, emb_buf, log_buf, piece_ref, token_ref, ga_ref, gx_ref, lx_ref, emb_sem, log_sem, own_sem, got_sem = refs
    core, start, _ = seat(out_ref.shape[0])
    half = ha_ref.shape[0]
    token_ref[...] = mark_ref[...]

    def fetch(k):
        slot = lax.rem(k, 2)
        mine = pl.ds(pl.multiple_of(k * CH, CH), CH)
        return (pltpu.make_async_copy(emb_ref.at[rows_at(core, k, 1)], emb_buf.at[slot], emb_sem),
                pltpu.make_async_copy(log_ref.at[mine], log_buf.at[slot], log_sem))

    writes = []
    if prev:
        writes.append(pltpu.make_async_copy(own_ref, out_ref.at[rows_at(core, *prev)], own_sem))
    if late:
        writes.append(pltpu.make_async_copy(got_ref, out_ref.at[rows_at(1 - core, *late)], got_sem))
    if not prev:
        for copy in fetch(jnp.int32(first)):
            copy.start()
    for copy in writes:
        copy.start()
    if job == 'act':
        norm_ref, *src = jobs_in
        for src_ref, dst_ref, turn_ref in zip(src, jobs_out[:2], jobs_out[2:]):
            dst_ref[...] = (src_ref[...] * norm_ref[...]).astype(BF16)
            turn_ref[...] = dst_ref[...].T
        hc_ref, hd_ref, xc_ref, xd_ref = jobs_out
    if job == 'add':
        jobs_out[0][...] = jobs_in[0][...] + jobs_in[1][...]
    if not prev:
        for copy in fetch(jnp.int32(first)):
            copy.wait()

    def step(i, carry):
        k = first + i
        slot = lax.rem(k, 2)
        rows = pl.ds(pl.multiple_of(i * CH, CH), CH)
        more = k + 1 < per_core

        @pl.when(more)
        def _():
            for copy in fetch(k + 1):
                copy.start()

        base = start + k * CH
        for side in (0, 1):
            cols = pl.ds(side * half, half)
            want = row_ref[2:3, cols].astype(jnp.int32) - base
            ga_ref[:, cols] = weights(log_buf[slot, :, cols], row_ref[0:1, cols], rows_of(CH, half, 0) == want, inv_n)
        for side, h_ref in ((0, xc_ref), (1, xd_ref)):
            cols = pl.ds(side * half, half)
            lx_ref[:, cols] = dot(emb_buf[slot], h_ref[...], NN)
        piece_ref[rows, :] = dot(ga_ref[:, pl.ds(0, half)], ha_ref[...], NN) + dot(ga_ref[:, pl.ds(half, half)], hb_ref[...], NN)
        for side in (0, 1):
            cols = pl.ds(side * half, half)
            want = rowx_ref[2:3, cols].astype(jnp.int32) - base
            gx_ref[:, cols] = weights(lx_ref[:, cols], rowx_ref[0:1, cols], rows_of(CH, half, 0) == want, inv_n)
        piece_ref[rows, :] += dot(gx_ref[:, pl.ds(0, half)], hc_ref[...], NN) + dot(gx_ref[:, pl.ds(half, half)], hd_ref[...], NN)

        @pl.when(more)
        def _():
            for copy in fetch(k + 1):
                copy.wait()

        return carry

    lax.fori_loop(0, count, step, 0)
    for copy in writes:
        copy.wait()


def tail_kernel(inv_n, vocab_loc, tail_ref, ha_ref, hb_ref, hc_ref, hd_ref, row_ref, rowx_ref, *refs):
    sums, (_, out_ref, sum_ref, loss_ref, g_ref) = refs[:4], refs[4:]
    half = ha_ref.shape[0]
    _, _, tail_base = seat(vocab_loc)
    both = (sums[0][...] + sums[1][...]) + (sums[2][...] + sums[3][...])
    sum_ref[...] = both[0:1]
    loss_ref[0, 0] = jnp.sum(both[1:2, 0:128]) * (inv_n / 256)
    grad = jnp.zeros(out_ref.shape, F32)
    ids = rows_of(TAIL, half, 0)
    for h_ref, r_ref, side in ((ha_ref, row_ref, 0), (hb_ref, row_ref, 1), (hc_ref, rowx_ref, 0), (hd_ref, rowx_ref, 1)):
        cols = pl.ds(side * half, half)
        logit = dot(tail_ref[...], h_ref[...], NT)
        g_ref[...] = weights(logit, r_ref[0:1, cols], ids + tail_base == r_ref[2:3, cols].astype(jnp.int32), inv_n)
        grad += dot(g_ref[...], h_ref[...], NN)
    out_ref[...] = grad


def last_kernel(places, _, *refs):
    srcs, out_ref, sems = refs[:len(places)], refs[len(places)], refs[len(places) + 1:]
    core, _, _ = seat(out_ref.shape[0])
    copies = []
    for src, sem, (other, place) in zip(srcs, sems, places):
        side = 1 - core if other else core
        copies.append(pltpu.make_async_copy(src, out_ref.at[rows_at(side, *place)], sem))
    for copy in copies:
        copy.start()
    for copy in copies:
        copy.wait()


def cost(flops, moved):
    return pl.CostEstimate(flops=int(flops), bytes_accessed=int(moved), transcendentals=0)


def params(mib):
    return pltpu.CompilerParams(vmem_limit_bytes=mib << 20)


def swapped(value, axis, perm):
    return lax.ppermute(value, axis, perm)


def solution(mesh):
    n_tp, n_dp = mesh.shape['tp'], mesh.shape['dp']

    def program(hidden, residual, targets, embedding, norm_w):
        inv_n = 1.0 / (hidden.shape[0] * hidden.shape[1])

        def local_part(hid_loc, res_loc, tgt_loc, emb_loc, norm_vec):
            n_batch, n_seq, d = hid_loc.shape
            half = n_batch * n_seq
            vocab_loc = emb_loc.shape[0]
            per_core = sum(PIECES)
            tail_rows = vocab_loc - 2 * per_core * CH
            my_dp = lax.axis_index('dp')
            core = lax.rem(my_dp, 2)
            core_arg = core.reshape(1)
            swap = [(i, i ^ 1) for i in range(n_dp)]
            cross = [(i, i ^ 2) for i in range(n_dp)]
            cross_swap = [(i, i ^ 3) for i in range(n_dp)]
            flip = [(i, i ^ 1) for i in range(n_tp)]
            flip_swap = [(t * n_dp + i, (t ^ 1) * n_dp + (i ^ 1)) for t in range(n_tp) for i in range(n_dp)]

            norm_row = norm_vec.reshape(1, d)
            tgt_own = tgt_loc.reshape(1, half)
            rows = half // 4
            scaled, ha, inv_rms = pl.pallas_call(
                norm_kernel,
                grid=(4,),
                in_specs=[pl.BlockSpec((rows, d), lambda i: (i, 0)), pl.BlockSpec((rows, d), lambda i: (i, 0)), VM],
                out_specs=[pl.BlockSpec((rows, d), lambda i: (i, 0)), pl.BlockSpec((rows, d), lambda i: (i, 0)), pl.BlockSpec((rows, 128), lambda i: (i, 0))],
                out_shape=[jax.ShapeDtypeStruct((half, d), F32), jax.ShapeDtypeStruct((half, d), BF16), jax.ShapeDtypeStruct((half, 128), F32)],
                compiler_params=params(14),
                cost_estimate=cost(1e7, half * d * 12),
            )(hid_loc.reshape(half, d), res_loc.reshape(half, d), norm_row)
            scaled_sib = lax.ppermute(scaled, 'dp', swap)
            tgt_sib = lax.ppermute(tgt_own, 'dp', swap)
            scaled_far = swapped(scaled, 'dp', cross)
            tgt_near = jnp.concatenate([tgt_own, tgt_sib], axis=1)
            emb_tail = jnp.pad(emb_loc[2 * per_core * CH:], ((0, TAIL - tail_rows), (0, 0)))

            steps, blk = per_core // STEP, STEP * CH
            flops_unit = 2.0 * CH * d * half
            logits, logits_tail, stat, hb = pl.pallas_call(
                functools.partial(stats_kernel, tail_rows),
                grid_spec=pltpu.PrefetchScalarGridSpec(
                    num_scalar_prefetch=1, grid=(steps,),
                    in_specs=[pl.BlockSpec((blk, d), lambda i, c: (c[0] * steps + i, 0)), VM, VM, VM, VM, VM],
                    out_specs=[pl.BlockSpec((blk, 2 * half), lambda i, c: (i, 0)), VM, VM, VM],
                    scratch_shapes=[pltpu.VMEM((8, 2 * half), F32)] * 3 + [pltpu.VMEM((d, half), BF16)] * 2),
                out_shape=[jax.ShapeDtypeStruct((per_core * CH, 2 * half), F32),
                           jax.ShapeDtypeStruct((TAIL, 2 * half), F32), jax.ShapeDtypeStruct((8, 2 * half), F32), jax.ShapeDtypeStruct((half, d), BF16)],
                compiler_params=params(30),
                cost_estimate=cost(flops_unit * per_core * 2, per_core * CH * (2 * d + 8 * half)),
            )(core_arg, emb_loc, emb_tail, ha, scaled_sib, norm_row, tgt_near)

            def turned(x):
                return jnp.concatenate([x[:, half:], x[:, :half]], axis=1)

            near = stat[0:3]
            sib = turned(lax.ppermute(near, 'dp', swap))
            over = lax.ppermute(near, 'tp', flip)
            over_sib = turned(lax.ppermute(near, ('tp', 'dp'), flip_swap))
            top = jnp.maximum(jnp.maximum(near[0], sib[0]), jnp.maximum(over[0], over_sib[0]))
            parts = [p[1] * jnp.exp(p[0] - top) for p in (near, sib, over, over_sib)]
            sum_exp = (parts[0] + parts[1]) + (parts[2] + parts[3])
            tgt_logit = (near[2] + sib[2]) + (over[2] + over_sib[2])
            token_loss = top + jnp.log(sum_exp) - tgt_logit
            row_near = jnp.pad(jnp.stack([jnp.log2(inv_n / sum_exp) - top * LOG2E, token_loss, tgt_near[0].astype(F32)]), ((0, 5), (0, 0)))
            row_near, scaled_far = lax.optimization_barrier((row_near, scaled_far))
            scaled_far_sib = swapped(scaled_far, 'dp', swap)
            row_far = swapped(row_near, 'dp', cross)

            dh_own, dh_sib, loss_chip = pl.pallas_call(
                functools.partial(dh_kernel, tail_rows, inv_n),
                grid_spec=pltpu.PrefetchScalarGridSpec(
                    num_scalar_prefetch=1, grid=(steps,),
                    in_specs=[pl.BlockSpec((blk, d), lambda i, c: (c[0] * steps + i, 0)),
                              pl.BlockSpec((blk, 2 * half), lambda i, c: (i, 0)), VM, VM, VM, VM],
                    out_specs=[VM, VM, VM],
                    scratch_shapes=[pltpu.VMEM((blk, 2 * half), BF16), pltpu.VMEM((TAIL, 2 * half), BF16)]),
                out_shape=[jax.ShapeDtypeStruct((half, d), F32)] * 2 + [jax.ShapeDtypeStruct((8, 128), F32)],
                compiler_params=params(31),
                cost_estimate=cost(flops_unit * per_core * 2, per_core * CH * (2 * d + 8 * half)),
            )(core_arg, emb_loc, logits, emb_tail, logits_tail, row_near, tgt_near)

            tie = lax.optimization_barrier
            row_near, row_far, scaled_far, scaled_far_sib, dh_own, dh_sib = tie(
                (row_near, row_far, scaled_far, scaled_far_sib, dh_own, dh_sib))
            dh_got = swapped(dh_sib, 'dp', swap)

            def piece_call(first, count, mark, out, bufs, prev, own, late, got, far, job, job_args, job_outs):
                extra = ([] if out is None else [out, *bufs, own]) + ([] if got is None else [got]) + job_args
                specs = ([] if out is None else [HB, VM, VM, VM]) + ([] if got is None else [VM]) + [VM] * len(job_args)
                return pl.pallas_call(
                    functools.partial(grad_kernel, job, first, count, prev, late, inv_n),
                    in_specs=[HB, HB] + [VM] * 9 + specs,
                    out_specs=[HB] + [VM] * (4 + len(job_outs)),
                    scratch_shapes=[pltpu.VMEM((CH, 2 * half), BF16), pltpu.VMEM((CH, 2 * half), BF16), pltpu.VMEM((CH, 2 * half), F32)]
                    + [pltpu.SemaphoreType.DMA] * 4,
                    out_shape=[jax.ShapeDtypeStruct((vocab_loc, d), F32), jax.ShapeDtypeStruct((2, CH, d), BF16),
                               jax.ShapeDtypeStruct((2, CH, 2 * half), F32), pltpu.VMEM((count * CH, d), F32),
                               jax.ShapeDtypeStruct((8, 128), F32)] + job_outs,
                    input_output_aliases={} if out is None else {11: 0, 12: 1, 13: 2},
                    compiler_params=params(8 if job is None else 10),
                    cost_estimate=cost(flops_unit * count * 6, count * CH * (2 * d + 8 * half + 8 * d)),
                )(emb_loc, logits, ha, hb, *far, row_near, row_far, mark, *extra)

            out, bufs, first, own, prev, arrived = None, (), 0, None, None, []
            mark = jnp.zeros((8, 128), F32)
            far = (ha, hb, ha, hb)
            for k, count in enumerate(PIECES):
                late, got = arrived[k - 2] if k >= 2 else (None, None)
                job, job_args, job_outs = None, [], []
                if k == 0:
                    job, job_args = 'act', [norm_row, scaled_far, scaled_far_sib]
                    job_outs = [jax.ShapeDtypeStruct((half, d), BF16)] * 2 + [jax.ShapeDtypeStruct((d, half), BF16)] * 2
                if k == ADD_AT:
                    dh_got, mark = tie((dh_got, mark))
                    job, job_args, job_outs = 'add', [dh_own, dh_got], [jax.ShapeDtypeStruct((half, d), F32)]
                out, emb_buf, log_buf, piece, mark, *made = piece_call(
                    first, count, mark, out, bufs, prev, own, late, got, far, job, job_args, job_outs)
                bufs = (emb_buf, log_buf)
                own, prev = piece, (first, count)
                arrived.append((prev, lax.ppermute(piece, 'dp', swap)))
                first += count
                if k == 0:
                    far = made
                if k == ADD_AT:
                    dh_chip, mark = tie((made[0], mark))
                    dh_far = swapped(dh_chip, 'tp', flip)
                if k == FINISH_AT:
                    dh_far, mark = tie((dh_far, mark))
                    blk_rows = pl.BlockSpec((half // 8, d), lambda i: (i, 0))
                    grad_r, grad_w = pl.pallas_call(
                        finish_kernel,
                        grid=(8,),
                        in_specs=[VM, pl.BlockSpec((half // 8, 128), lambda i: (i, 0)), VM, blk_rows, blk_rows, blk_rows],
                        out_specs=[blk_rows, VM],
                        scratch_shapes=[pltpu.VMEM((8, d), F32)],
                        out_shape=[jax.ShapeDtypeStruct((half, d), F32), jax.ShapeDtypeStruct((2, d), F32)],
                        compiler_params=params(4),
                        cost_estimate=cost(1e7, half * d * 16),
                    )(norm_row, inv_rms, loss_chip, scaled, dh_chip, dh_far)
                    grad_w, mark = tie((grad_w, mark))
                    gw = [swapped(grad_w, 'dp', swap), swapped(grad_w, 'dp', cross), swapped(grad_w, 'dp', cross_swap)]
            hc, hd = far[:2]

            out, grad_w, loss_mean = pl.pallas_call(
                functools.partial(tail_kernel, inv_n, vocab_loc),
                grid=(1,), in_specs=[VM] * 11 + [HB],
                out_specs=[pl.BlockSpec((TAIL, d), lambda i: (2 * per_core * CH // TAIL, 0)), VM, pl.BlockSpec(memory_space=pltpu.SMEM)],
                scratch_shapes=[pltpu.VMEM((TAIL, half), BF16)],
                out_shape=[jax.ShapeDtypeStruct((vocab_loc, d), F32), jax.ShapeDtypeStruct((1, d), F32), jax.ShapeDtypeStruct((1, 1), F32)],
                input_output_aliases={11: 0},
                compiler_params=params(14),
                cost_estimate=cost(2.0 * TAIL * d * half * 8, 4 * TAIL * d),
            )(emb_tail, ha, hb, hc, hd, row_near, row_far, grad_w, *gw, out)
            for parts in ([(False, prev, own), (True, *arrived[-2]), (True, *arrived[-1])],):
                out = pl.pallas_call(
                    functools.partial(last_kernel, [p[:2] for p in parts]),
                    in_specs=[HB] + [VM] * len(parts), out_specs=HB,
                    scratch_shapes=[pltpu.SemaphoreType.DMA] * len(parts),
                    out_shape=jax.ShapeDtypeStruct((vocab_loc, d), F32),
                    input_output_aliases={0: 0},
                    compiler_params=params(8),
                    cost_estimate=cost(1e6, sum(4 * p[1][1] * CH * d for p in parts)),
                )(out, *[p[2] for p in parts])
            return loss_mean.reshape(()), grad_r.reshape(n_batch, n_seq, d), out, grad_w.reshape(d)

        sharded = jax.shard_map(
            local_part, mesh=mesh,
            in_specs=(P('dp', None, None), P('dp', None, None), P('dp', None), P('tp', None), P(None)),
            out_specs=(P(), P('dp', None, None), P('tp', None), P(None)),
            check_vma=False)
        return sharded(hidden, residual, targets, embedding, norm_w)

    return program
```

```python
import functools

import jax
import jax.numpy as jnp
from jax import lax
from jax.experimental import pallas as pl
from jax.experimental.pallas import tpu as pltpu
from jax.sharding import PartitionSpec as P


NORM_EPS = 1e-5
CH = 256
STEP = 7
GROUPS = (1, 2, 2, 2)
PIECES = (5, 5, 5, 6, 5, 6, 5, 6, 4, 2)
ADD_AT, FINISH_AT = 1, 5
TAIL = 64
F32, BF16 = jnp.float32, jnp.bfloat16
NN = (((1,), (0,)), ((), ()))
NT = (((1,), (1,)), ((), ()))
TN = (((0,), (0,)), ((), ()))
VM = pl.BlockSpec(memory_space=pltpu.VMEM)
HB = pl.BlockSpec(memory_space=pl.ANY)


def dot(a, b, dims):
    return lax.dot_general(a, b, dims, preferred_element_type=F32)


LOG2E = 1.4426950408889634


def weights(logit, shift, hit, inv_n):
    return (jnp.exp2(logit * LOG2E + shift) - jnp.where(hit, inv_n, 0.0)).astype(BF16)


def seat(vocab_loc):
    core, start, span = lax.rem(lax.axis_index('dp'), 2), lax.axis_index('tp') * vocab_loc, sum(PIECES) * CH
    return core, start + core * span, start + 2 * span


def rows_of(n, width, base):
    return lax.broadcasted_iota(jnp.int32, (n, width), 0) + base


def norm_kernel(hid_ref, res_ref, norm_ref, scaled_ref, act_ref, inv_ref):
    resid = res_ref[...] + hid_ref[...].astype(F32)
    inv = lax.rsqrt(jnp.mean(resid * resid, axis=-1, keepdims=True) + NORM_EPS)
    scaled = resid * inv
    scaled_ref[...] = scaled
    act_ref[...] = (scaled * norm_ref[...]).astype(BF16)
    inv_ref[...] = jnp.broadcast_to(inv, inv_ref.shape)


def stats_kernel(tail_rows, core_ref, emb_ref, tail_ref, ha_ref, sib_ref, norm_ref, tgt_ref, log_ref, logt_ref, stat_ref, hb_ref, top, total, hits, wa_ref, wb_ref):
    step = pl.program_id(0)
    core, base, tail_base = seat(2 * sum(PIECES) * CH + tail_rows)
    half = ha_ref.shape[0]

    @pl.when(step == 0)
    def _():
        top[...] = jnp.full_like(top, -jnp.inf)
        total[...] = jnp.zeros_like(total)
        hits[...] = jnp.zeros_like(hits)
        hb_ref[...] = (sib_ref[...] * norm_ref[...]).astype(BF16)
        wa_ref[...] = ha_ref[...].T
        wb_ref[...] = hb_ref[...].T

    def fold(cols, logit, hit):
        split = logit.reshape(-1, 8, half)
        new = jnp.maximum(top[:, cols], jnp.max(split, axis=0))
        total[:, cols] = total[:, cols] * jnp.exp(top[:, cols] - new) + jnp.sum(jnp.exp(split - new[None]), axis=0)
        top[:, cols] = new
        hits[:, cols] += jnp.sum(jnp.where(hit, logit, 0.0).reshape(-1, 8, half), axis=0)

    for k in range(STEP):
        rows = pl.ds(k * CH, CH)
        for side, h_ref in ((0, wa_ref), (1, wb_ref)):
            cols = pl.ds(side * half, half)
            logit = dot(emb_ref[rows, :], h_ref[...], NN)
            log_ref[rows, cols] = logit
            want = tgt_ref[0:1, cols] - (base + (step * STEP + k) * CH)
            fold(cols, logit, rows_of(CH, half, 0) == want)

    @pl.when(step == pl.num_programs(0) - 1)
    def _():
        for side, h_ref in ((0, wa_ref), (1, wb_ref)):
            cols = pl.ds(side * half, half)
            ids = rows_of(TAIL, half, 0)
            live = jnp.logical_and(ids < tail_rows, core == 0)
            logit = jnp.where(live, dot(tail_ref[...], h_ref[...], NN), -jnp.inf)
            logt_ref[:, cols] = logit
            fold(cols, logit, jnp.logical_and(ids + tail_base == tgt_ref[0:1, cols], live))
        peak = jnp.max(top[...], axis=0, keepdims=True)
        stat_ref[...] = jnp.zeros_like(stat_ref)
        stat_ref[0:1, :] = peak
        stat_ref[1:2, :] = jnp.sum(total[...] * jnp.exp(top[...] - peak), axis=0, keepdims=True)
        stat_ref[2:3, :] = jnp.sum(hits[...], axis=0, keepdims=True)


def dh_kernel(tail_rows, inv_n, core_ref, emb_ref, log_ref, tail_ref, logt_ref, row_ref, tgt_ref, da_ref, db_ref, loss_ref, g_ref, gt_ref):
    step = pl.program_id(0)
    core, base, tail_base = seat(2 * sum(PIECES) * CH + tail_rows)
    half = da_ref.shape[0]

    @pl.when(step == 0)
    def _():
        loss_ref[...] = jnp.full(loss_ref.shape, jnp.sum(row_ref[1:2, pl.ds(0, half)]) + jnp.sum(row_ref[1:2, pl.ds(half, half)]))
        da_ref[...] = jnp.zeros_like(da_ref)
        db_ref[...] = jnp.zeros_like(db_ref)

    k = 0
    for group in GROUPS:
        for side, d_ref in ((0, da_ref), (1, db_ref)):
            cols = pl.ds(side * half, half)
            for i in range(k, k + group):
                rows = pl.ds(i * CH, CH)
                want = tgt_ref[0:1, cols] - (base + (step * STEP + i) * CH)
                g_ref[rows, cols] = weights(log_ref[rows, cols], row_ref[0:1, cols], rows_of(CH, half, 0) == want, inv_n)
            rows = pl.ds(k * CH, group * CH)
            d_ref[...] += dot(g_ref[rows, cols], emb_ref[rows, :], TN)
        k += group

    @pl.when(step == pl.num_programs(0) - 1)
    def _():
        for side, d_ref in ((0, da_ref), (1, db_ref)):
            cols = pl.ds(side * half, half)
            ids = rows_of(TAIL, half, 0)
            live = jnp.logical_and(ids < tail_rows, core == 0)
            hit = jnp.logical_and(ids + tail_base == tgt_ref[0:1, cols], live)
            gt_ref[:, cols] = weights(logt_ref[:, cols], row_ref[0:1, cols], hit, inv_n)
            d_ref[...] += dot(gt_ref[:, cols], tail_ref[...], TN)


JOBS = {None: (0, 0), 'act': (3, 4), 'add': (2, 1)}


def finish_kernel(norm_ref, inv_ref, loss_ref, scaled_ref, near_ref, far_ref, grad_ref, sum_ref, total_ref):
    @pl.when(pl.program_id(0) == 0)
    def _():
        total_ref[...] = jnp.zeros_like(total_ref)

    grad_h, scaled = near_ref[...] + far_ref[...], scaled_ref[...]
    total_ref[...] += jnp.sum((grad_h * scaled).reshape(-1, 8, scaled.shape[1]), axis=0)
    grad_scaled = grad_h * norm_ref[...]
    mean = jnp.mean(grad_scaled * scaled, axis=-1, keepdims=True)
    grad_ref[...] = inv_ref[:, 0:1] * (grad_scaled - scaled * mean)
    sum_ref[0:1, :] = jnp.sum(total_ref[...], axis=0, keepdims=True)
    sum_ref[1:2, :] = jnp.zeros((1, sum_ref.shape[1]), F32)
    sum_ref[1:2, 0:128] = loss_ref[0:1, :]


def rows_at(core, first, count):
    return pl.ds(pl.multiple_of((core * sum(PIECES) + first) * CH, CH), count * CH)


def grad_kernel(job, first, count, prev, late, inv_n, emb_ref, log_ref, ha_ref, hb_ref, hc_ref, hd_ref, xc_ref, xd_ref, row_ref, rowx_ref, mark_ref, *refs):
    per_core = sum(PIECES)
    refs = list(refs)
    if prev:
        refs = refs[3:]
    own_ref = refs.pop(0) if prev else None
    got_ref = refs.pop(0) if late else None
    jobs_in = [refs.pop(0) for _ in range(JOBS[job][0])]
    jobs_out = [refs.pop(5) for _ in range(JOBS[job][1])]
    out_ref, emb_buf, log_buf, piece_ref, token_ref, ga_ref, gx_ref, lx_ref, emb_sem, log_sem, own_sem, got_sem = refs
    core, start, _ = seat(out_ref.shape[0])
    half = ha_ref.shape[0]
    token_ref[...] = mark_ref[...]

    def fetch(k):
        slot = lax.rem(k, 2)
        mine = pl.ds(pl.multiple_of(k * CH, CH), CH)
        return (pltpu.make_async_copy(emb_ref.at[rows_at(core, k, 1)], emb_buf.at[slot], emb_sem),
                pltpu.make_async_copy(log_ref.at[mine], log_buf.at[slot], log_sem))

    writes = []
    if prev:
        writes.append(pltpu.make_async_copy(own_ref, out_ref.at[rows_at(core, *prev)], own_sem))
    if late:
        writes.append(pltpu.make_async_copy(got_ref, out_ref.at[rows_at(1 - core, *late)], got_sem))
    if not prev:
        for copy in fetch(jnp.int32(first)):
            copy.start()
    for copy in writes:
        copy.start()
    if job == 'act':
        norm_ref, *src = jobs_in
        for src_ref, dst_ref, turn_ref in zip(src, jobs_out[:2], jobs_out[2:]):
            dst_ref[...] = (src_ref[...] * norm_ref[...]).astype(BF16)
            turn_ref[...] = dst_ref[...].T
        hc_ref, hd_ref, xc_ref, xd_ref = jobs_out
    if job == 'add':
        jobs_out[0][...] = jobs_in[0][...] + jobs_in[1][...]
    if not prev:
        for copy in fetch(jnp.int32(first)):
            copy.wait()

    def step(i, carry):
        k = first + i
        slot = lax.rem(k, 2)
        rows = pl.ds(pl.multiple_of(i * CH, CH), CH)
        more = k + 1 < per_core

        @pl.when(more)
        def _():
            for copy in fetch(k + 1):
                copy.start()

        base = start + k * CH
        for side in (0, 1):
            cols = pl.ds(side * half, half)
            want = row_ref[2:3, cols].astype(jnp.int32) - base
            ga_ref[:, cols] = weights(log_buf[slot, :, cols], row_ref[0:1, cols], rows_of(CH, half, 0) == want, inv_n)
        for side, h_ref in ((0, xc_ref), (1, xd_ref)):
            cols = pl.ds(side * half, half)
            lx_ref[:, cols] = dot(emb_buf[slot], h_ref[...], NN)
        piece_ref[rows, :] = dot(ga_ref[:, pl.ds(0, half)], ha_ref[...], NN) + dot(ga_ref[:, pl.ds(half, half)], hb_ref[...], NN)
        for side in (0, 1):
            cols = pl.ds(side * half, half)
            want = rowx_ref[2:3, cols].astype(jnp.int32) - base
            gx_ref[:, cols] = weights(lx_ref[:, cols], rowx_ref[0:1, cols], rows_of(CH, half, 0) == want, inv_n)
        piece_ref[rows, :] += dot(gx_ref[:, pl.ds(0, half)], hc_ref[...], NN) + dot(gx_ref[:, pl.ds(half, half)], hd_ref[...], NN)

        @pl.when(more)
        def _():
            for copy in fetch(k + 1):
                copy.wait()

        return carry

    lax.fori_loop(0, count, step, 0)
    for copy in writes:
        copy.wait()


def tail_kernel(inv_n, vocab_loc, tail_ref, ha_ref, hb_ref, hc_ref, hd_ref, row_ref, rowx_ref, *refs):
    sums, (_, out_ref, sum_ref, loss_ref, g_ref) = refs[:4], refs[4:]
    half = ha_ref.shape[0]
    _, _, tail_base = seat(vocab_loc)
    both = (sums[0][...] + sums[1][...]) + (sums[2][...] + sums[3][...])
    sum_ref[...] = both[0:1]
    loss_ref[0, 0] = jnp.sum(both[1:2, 0:128]) * (inv_n / 256)
    grad = jnp.zeros(out_ref.shape, F32)
    ids = rows_of(TAIL, half, 0)
    for h_ref, r_ref, side in ((ha_ref, row_ref, 0), (hb_ref, row_ref, 1), (hc_ref, rowx_ref, 0), (hd_ref, rowx_ref, 1)):
        cols = pl.ds(side * half, half)
        logit = dot(tail_ref[...], h_ref[...], NT)
        g_ref[...] = weights(logit, r_ref[0:1, cols], ids + tail_base == r_ref[2:3, cols].astype(jnp.int32), inv_n)
        grad += dot(g_ref[...], h_ref[...], NN)
    out_ref[...] = grad


def last_kernel(places, _, *refs):
    srcs, out_ref, sems = refs[:len(places)], refs[len(places)], refs[len(places) + 1:]
    core, _, _ = seat(out_ref.shape[0])
    copies = []
    for src, sem, (other, place) in zip(srcs, sems, places):
        side = 1 - core if other else core
        copies.append(pltpu.make_async_copy(src, out_ref.at[rows_at(side, *place)], sem))
    for copy in copies:
        copy.start()
    for copy in copies:
        copy.wait()


def cost(flops, moved):
    return pl.CostEstimate(flops=int(flops), bytes_accessed=int(moved), transcendentals=0)


def params(mib):
    return pltpu.CompilerParams(vmem_limit_bytes=mib << 20)


def swapped(value, axis, perm):
    return lax.ppermute(value, axis, perm)


def solution(mesh):
    n_tp, n_dp = mesh.shape['tp'], mesh.shape['dp']

    def program(hidden, residual, targets, embedding, norm_w):
        inv_n = 1.0 / (hidden.shape[0] * hidden.shape[1])

        def local_part(hid_loc, res_loc, tgt_loc, emb_loc, norm_vec):
            n_batch, n_seq, d = hid_loc.shape
            half = n_batch * n_seq
            vocab_loc = emb_loc.shape[0]
            per_core = sum(PIECES)
            tail_rows = vocab_loc - 2 * per_core * CH
            my_dp = lax.axis_index('dp')
            core = lax.rem(my_dp, 2)
            core_arg = core.reshape(1)
            swap = [(i, i ^ 1) for i in range(n_dp)]
            cross = [(i, i ^ 2) for i in range(n_dp)]
            cross_swap = [(i, i ^ 3) for i in range(n_dp)]
            flip = [(i, i ^ 1) for i in range(n_tp)]
            flip_swap = [(t * n_dp + i, (t ^ 1) * n_dp + (i ^ 1)) for t in range(n_tp) for i in range(n_dp)]

            norm_row = norm_vec.reshape(1, d)
            tgt_own = tgt_loc.reshape(1, half)
            rows = half // 4
            scaled, ha, inv_rms = pl.pallas_call(
                norm_kernel,
                grid=(4,),
                in_specs=[pl.BlockSpec((rows, d), lambda i: (i, 0)), pl.BlockSpec((rows, d), lambda i: (i, 0)), VM],
                out_specs=[pl.BlockSpec((rows, d), lambda i: (i, 0)), pl.BlockSpec((rows, d), lambda i: (i, 0)), pl.BlockSpec((rows, 128), lambda i: (i, 0))],
                out_shape=[jax.ShapeDtypeStruct((half, d), F32), jax.ShapeDtypeStruct((half, d), BF16), jax.ShapeDtypeStruct((half, 128), F32)],
                compiler_params=params(56),
                cost_estimate=cost(1e7, half * d * 12),
            )(hid_loc.reshape(half, d), res_loc.reshape(half, d), norm_row)
            scaled_sib = lax.ppermute(scaled, 'dp', swap)
            tgt_sib = lax.ppermute(tgt_own, 'dp', swap)
            scaled_far = swapped(scaled, 'dp', cross)
            tgt_near = jnp.concatenate([tgt_own, tgt_sib], axis=1)
            emb_tail = jnp.pad(emb_loc[2 * per_core * CH:], ((0, TAIL - tail_rows), (0, 0)))

            steps, blk = per_core // STEP, STEP * CH
            flops_unit = 2.0 * CH * d * half
            logits, logits_tail, stat, hb = pl.pallas_call(
                functools.partial(stats_kernel, tail_rows),
                grid_spec=pltpu.PrefetchScalarGridSpec(
                    num_scalar_prefetch=1, grid=(steps,),
                    in_specs=[pl.BlockSpec((blk, d), lambda i, c: (c[0] * steps + i, 0)), VM, VM, VM, VM, VM],
                    out_specs=[pl.BlockSpec((blk, 2 * half), lambda i, c: (i, 0)), VM, VM, VM],
                    scratch_shapes=[pltpu.VMEM((8, 2 * half), F32)] * 3 + [pltpu.VMEM((d, half), BF16)] * 2),
                out_shape=[jax.ShapeDtypeStruct((per_core * CH, 2 * half), F32),
                           jax.ShapeDtypeStruct((TAIL, 2 * half), F32), jax.ShapeDtypeStruct((8, 2 * half), F32), jax.ShapeDtypeStruct((half, d), BF16)],
                compiler_params=params(30),
                cost_estimate=cost(flops_unit * per_core * 2, per_core * CH * (2 * d + 8 * half)),
            )(core_arg, emb_loc, emb_tail, ha, scaled_sib, norm_row, tgt_near)

            def turned(x):
                return jnp.concatenate([x[:, half:], x[:, :half]], axis=1)

            near = stat[0:3]
            sib = turned(lax.ppermute(near, 'dp', swap))
            over = lax.ppermute(near, 'tp', flip)
            over_sib = turned(lax.ppermute(near, ('tp', 'dp'), flip_swap))
            top = jnp.maximum(jnp.maximum(near[0], sib[0]), jnp.maximum(over[0], over_sib[0]))
            parts = [p[1] * jnp.exp(p[0] - top) for p in (near, sib, over, over_sib)]
            sum_exp = (parts[0] + parts[1]) + (parts[2] + parts[3])
            tgt_logit = (near[2] + sib[2]) + (over[2] + over_sib[2])
            token_loss = top + jnp.log(sum_exp) - tgt_logit
            row_near = jnp.pad(jnp.stack([jnp.log2(inv_n / sum_exp) - top * LOG2E, token_loss, tgt_near[0].astype(F32)]), ((0, 5), (0, 0)))
            row_near, scaled_far = lax.optimization_barrier((row_near, scaled_far))
            scaled_far_sib = swapped(scaled_far, 'dp', swap)
            row_far = swapped(row_near, 'dp', cross)

            dh_own, dh_sib, loss_chip = pl.pallas_call(
                functools.partial(dh_kernel, tail_rows, inv_n),
                grid_spec=pltpu.PrefetchScalarGridSpec(
                    num_scalar_prefetch=1, grid=(steps,),
                    in_specs=[pl.BlockSpec((blk, d), lambda i, c: (c[0] * steps + i, 0)),
                              pl.BlockSpec((blk, 2 * half), lambda i, c: (i, 0)), VM, VM, VM, VM],
                    out_specs=[VM, VM, VM],
                    scratch_shapes=[pltpu.VMEM((blk, 2 * half), BF16), pltpu.VMEM((TAIL, 2 * half), BF16)]),
                out_shape=[jax.ShapeDtypeStruct((half, d), F32)] * 2 + [jax.ShapeDtypeStruct((8, 128), F32)],
                compiler_params=params(31),
                cost_estimate=cost(flops_unit * per_core * 2, per_core * CH * (2 * d + 8 * half)),
            )(core_arg, emb_loc, logits, emb_tail, logits_tail, row_near, tgt_near)

            tie = lax.optimization_barrier
            row_near, row_far, scaled_far, scaled_far_sib, dh_own, dh_sib = tie(
                (row_near, row_far, scaled_far, scaled_far_sib, dh_own, dh_sib))
            dh_got = swapped(dh_sib, 'dp', swap)

            def piece_call(first, count, mark, out, bufs, prev, own, late, got, far, job, job_args, job_outs):
                extra = ([] if out is None else [out, *bufs, own]) + ([] if got is None else [got]) + job_args
                specs = ([] if out is None else [HB, VM, VM, VM]) + ([] if got is None else [VM]) + [VM] * len(job_args)
                return pl.pallas_call(
                    functools.partial(grad_kernel, job, first, count, prev, late, inv_n),
                    in_specs=[HB, HB] + [VM] * 9 + specs,
                    out_specs=[HB] + [VM] * (4 + len(job_outs)),
                    scratch_shapes=[pltpu.VMEM((CH, 2 * half), BF16), pltpu.VMEM((CH, 2 * half), BF16), pltpu.VMEM((CH, 2 * half), F32)]
                    + [pltpu.SemaphoreType.DMA] * 4,
                    out_shape=[jax.ShapeDtypeStruct((vocab_loc, d), F32), jax.ShapeDtypeStruct((2, CH, d), BF16),
                               jax.ShapeDtypeStruct((2, CH, 2 * half), F32), pltpu.VMEM((count * CH, d), F32),
                               jax.ShapeDtypeStruct((8, 128), F32)] + job_outs,
                    input_output_aliases={} if out is None else {11: 0, 12: 1, 13: 2},
                    compiler_params=params(8 if job is None else 10),
                    cost_estimate=cost(flops_unit * count * 6, count * CH * (2 * d + 8 * half + 8 * d)),
                )(emb_loc, logits, ha, hb, *far, row_near, row_far, mark, *extra)

            out, bufs, first, own, prev, arrived = None, (), 0, None, None, []
            mark = jnp.zeros((8, 128), F32)
            far = (ha, hb, ha, hb)
            for k, count in enumerate(PIECES):
                late, got = arrived[k - 2] if k >= 2 else (None, None)
                job, job_args, job_outs = None, [], []
                if k == 0:
                    job, job_args = 'act', [norm_row, scaled_far, scaled_far_sib]
                    job_outs = [jax.ShapeDtypeStruct((half, d), BF16)] * 2 + [jax.ShapeDtypeStruct((d, half), BF16)] * 2
                if k == ADD_AT:
                    dh_got, mark = tie((dh_got, mark))
                    job, job_args, job_outs = 'add', [dh_own, dh_got], [jax.ShapeDtypeStruct((half, d), F32)]
                out, emb_buf, log_buf, piece, mark, *made = piece_call(
                    first, count, mark, out, bufs, prev, own, late, got, far, job, job_args, job_outs)
                bufs = (emb_buf, log_buf)
                own, prev = piece, (first, count)
                arrived.append((prev, swapped(piece, 'dp', swap)))
                first += count
                if k == 0:
                    far = made
                if k == ADD_AT:
                    dh_chip, mark = tie((made[0], mark))
                    dh_far = swapped(dh_chip, 'tp', flip)
                if k == FINISH_AT:
                    dh_far, mark = tie((dh_far, mark))
                    blk_rows = pl.BlockSpec((half // 4, d), lambda i: (i, 0))
                    grad_r, grad_w = pl.pallas_call(
                        finish_kernel,
                        grid=(4,),
                        in_specs=[VM, pl.BlockSpec((half // 4, 128), lambda i: (i, 0)), VM, blk_rows, blk_rows, blk_rows],
                        out_specs=[blk_rows, VM],
                        scratch_shapes=[pltpu.VMEM((8, d), F32)],
                        out_shape=[jax.ShapeDtypeStruct((half, d), F32), jax.ShapeDtypeStruct((2, d), F32)],
                        compiler_params=params(5),
                        cost_estimate=cost(1e7, half * d * 16),
                    )(norm_row, inv_rms, loss_chip, scaled, dh_chip, dh_far)
                    grad_w, mark = tie((grad_w, mark))
                    gw = [swapped(grad_w, 'dp', swap), swapped(grad_w, 'dp', cross), swapped(grad_w, 'dp', cross_swap)]
            hc, hd = far[:2]

            out, grad_w, loss_mean = pl.pallas_call(
                functools.partial(tail_kernel, inv_n, vocab_loc),
                grid=(1,), in_specs=[VM] * 11 + [HB],
                out_specs=[pl.BlockSpec((TAIL, d), lambda i: (2 * per_core * CH // TAIL, 0)), VM, pl.BlockSpec(memory_space=pltpu.SMEM)],
                scratch_shapes=[pltpu.VMEM((TAIL, half), BF16)],
                out_shape=[jax.ShapeDtypeStruct((vocab_loc, d), F32), jax.ShapeDtypeStruct((1, d), F32), jax.ShapeDtypeStruct((1, 1), F32)],
                input_output_aliases={11: 0},
                compiler_params=params(14),
                cost_estimate=cost(2.0 * TAIL * d * half * 8, 4 * TAIL * d),
            )(emb_tail, ha, hb, hc, hd, row_near, row_far, grad_w, *gw, out)
            for parts in ([(False, prev, own), (True, *arrived[-2]), (True, *arrived[-1])],):
                out = pl.pallas_call(
                    functools.partial(last_kernel, [p[:2] for p in parts]),
                    in_specs=[HB] + [VM] * len(parts), out_specs=HB,
                    scratch_shapes=[pltpu.SemaphoreType.DMA] * len(parts),
                    out_shape=jax.ShapeDtypeStruct((vocab_loc, d), F32),
                    input_output_aliases={0: 0},
                    compiler_params=params(8),
                    cost_estimate=cost(1e6, sum(4 * p[1][1] * CH * d for p in parts)),
                )(out, *[p[2] for p in parts])
            return loss_mean.reshape(()), grad_r.reshape(n_batch, n_seq, d), out, grad_w.reshape(d)

        sharded = jax.shard_map(
            local_part, mesh=mesh,
            in_specs=(P('dp', None, None), P('dp', None, None), P('dp', None), P('tp', None), P(None)),
            out_specs=(P(), P('dp', None, None), P('tp', None), P(None)),
            check_vma=False)
        return sharded(hidden, residual, targets, embedding, norm_w)

    return program
```
